128 devices in a mesh: dp: 16 (over y_hi, x, core), mp: 8 (over z, y_lo).
Axes of the slice: x: 4, y: 4 (y_hi: 2, y_lo: 2; y = y_hi * 2 + y_lo), z: 4, core: 2. Of those that a mesh axis runs over, the one named last changes fastest.
Arguments:
- hidden_states: bfloat16 [65536, 4096], P('dp', 'mp'), may hold values from -1 to 1
- factor_values: bfloat16 [65536, 128], P('dp', 'mp'), may hold values from 0.029907227 to 0.13964844
- class_ids: int32 [65536, 128], P('dp', 'mp'), may hold values from 0 to 128255, as said below
- centers: int32 [3], replicated, may hold values from 0 to 65535
Outputs:
- min_distance: float32 [65536], P(('dp', 'mp'))
- weight_means: float32 [3], replicated
The draws below stay inside these ranges and needn't reach their ends.
Inputs may be any that keep to these rules, and one draw needn't show every extreme that they name: `centers`: each value is a sample index. `class_ids`: entries k * 16 to (k + 1) * 16 - 1 of a row hold distinct classes of the k-th of 8 equal ranges of the vocabulary.
All inputs are finite; a program needn't handle non-finite values.
Results may differ from the reference program's by a relative error of at most 0.00095.
Values may be sent and summed in bfloat16 or wider, within the bound.
No kernel may reach another device: no remote copies, remote signals or barrier semaphores. Data moves between devices by JAX's collectives and lax.ppermute only.
A program may use at most 64 MiB of HBM per device.

```python
import jax
import jax.numpy as jnp
from jax import lax

D = 4096
VOCAB = 128256
K_LOC = 16
STEPS = 3
SAMP_DEV = 512
TOPK = 128
POOL = 65536


def draw_hidden_states(key, part):
    key_shared, key_noise = jax.random.split(key, 2)
    shared = jax.random.normal(key_shared, (1, D), jnp.float32)
    noise = jax.random.normal(key_noise, (POOL, D), jnp.float32)
    base = 0.7 * shared + 0.7 * noise
    return jnp.clip(base / jnp.sqrt(jnp.float32(D)), -1.0, 1.0).astype(jnp.bfloat16)


def draw_class_ids(key, part):
    nblk = TOPK // K_LOC
    span = VOCAB // nblk
    stride = span // K_LOC
    key_order, key_pick, key_near, key_far = jax.random.split(key, 4)
    scores = jax.random.randint(key_order, (POOL, nblk, K_LOC), 0, 1 << 20) * K_LOC + jnp.arange(K_LOC, dtype=jnp.int32)
    slots = jnp.argsort(scores, axis=-1, stable=True).astype(jnp.int32)
    pick = jax.random.randint(key_pick, (POOL, nblk, K_LOC), 0, 4)
    near = jax.random.randint(key_near, (POOL, nblk, K_LOC), 0, 4)
    far = jax.random.randint(key_far, (POOL, nblk, K_LOC), 0, stride)
    offset = jnp.where(pick > 0, near, far)
    base = (jnp.arange(nblk, dtype=jnp.int32) * span).reshape(1, nblk, 1)
    ids = base + slots * stride + offset
    return ids.reshape(POOL, TOPK).astype(jnp.int32)


def levels(own_key, shape, cuts, smallest, high):
    level, own = 1.0, jax.random.fold_in(own_key, 6)
    for dim, shards_of in cuts:
        heights = jnp.exp(jax.random.uniform(jax.random.fold_in(own, dim), (shards_of,), jnp.float32, smallest / len(cuts), high / len(cuts)))
        level = level * jnp.repeat(heights, shape[dim] // shards_of).reshape([-1 if axis == dim else 1 for axis in range(len(shape))])
    return level


def setup_inputs(seed: int = 0) -> dict:
    key_list = jax.random.split(jax.random.key(seed), 5)
    hidden_states = draw_hidden_states(jax.random.fold_in(key_list[4], 71), 0)
    factor_values = jnp.clip(0.029907227 + 0.10974121 * jax.random.uniform(key_list[1], (POOL, TOPK), jnp.float32) ** levels(key_list[1], (POOL, TOPK), ((0, 16), (1, 8)), -0.2, 0.2), 0.029907227, 0.13964844).astype(jnp.bfloat16)
    class_ids = draw_class_ids(jax.random.fold_in(key_list[4], 71), 0)
    centers = jax.random.randint(key_list[3], (STEPS,), 0, POOL).astype(jnp.int32)
    return {"hidden_states": hidden_states, "factor_values": factor_values, "class_ids": class_ids, "centers": centers}


def reference(hidden_states, factor_values, class_ids, centers):
    nblk = TOPK // K_LOC
    vals = factor_values.astype(jnp.float32)
    sq_h = jnp.sum(jnp.square(hidden_states.astype(jnp.float32)), axis=1)
    sq_a = jnp.sum(vals * vals, axis=1)
    groups = POOL // SAMP_DEV
    means = []
    min_distance = None
    for step in range(STEPS):
        center = centers[step].astype(jnp.int32)
        h_row = lax.dynamic_slice_in_dim(hidden_states, center, 1, 0)[0]
        v_row = lax.dynamic_slice_in_dim(vals, center, 1, 0)[0]
        i_row = lax.dynamic_slice_in_dim(class_ids, center, 1, 0)[0]
        inner_h = jnp.dot(hidden_states, h_row, preferred_element_type=jnp.float32)

        def block(pair):
            values, idents = pair
            match = idents.reshape(-1, nblk, K_LOC, 1) == i_row.reshape(1, nblk, 1, K_LOC)
            prod = values.reshape(-1, nblk, K_LOC, 1) * v_row.reshape(1, nblk, 1, K_LOC)
            return jnp.sum(jnp.where(match, prod, jnp.float32(0.0)), axis=(1, 2, 3))

        inner_a = lax.map(block, (vals.reshape(groups, SAMP_DEV, TOPK), class_ids.reshape(groups, SAMP_DEV, TOPK))).reshape(POOL)
        norm_hc = jnp.sum(jnp.square(h_row.astype(jnp.float32)))
        norm_ac = jnp.sum(v_row * v_row)
        dist = jnp.maximum(sq_h * sq_a + norm_hc * norm_ac - 2.0 * inner_h * inner_a, jnp.float32(0.0))
        min_distance = dist if step == 0 else jnp.minimum(min_distance, dist)
        means.append(jnp.sum(min_distance) / POOL)
    return min_distance, jnp.stack(means)
```

```python
import functools

import jax
import jax.numpy as jnp
from jax import lax
from jax.experimental import pallas as pl
from jax.experimental.pallas import tpu as pltpu
from jax.sharding import Mesh
from jax.sharding import PartitionSpec as P

K_LOC = 16
STEPS = 3
LANES = 128
MP = ("mp_0", "mp_1")
DP = ("dp_0", "dp_1", "dp_2")
DP_MP = ("dp_0", "dp_1", "dp_2", "mp_0", "mp_1")
VMEM = pltpu.VMEM
F32 = jnp.float32
BF16 = jnp.bfloat16


def vspec():
    return pl.BlockSpec(memory_space=VMEM)


def params(mib):
    return pltpu.CompilerParams(vmem_limit_bytes=mib * 1024 * 1024)


def pick_kernel(centers, hid, val, ids, out, hbuf, vbuf, ibuf, rows, sem):
    rows_all = hid.shape[0]
    copies = []
    for t in range(STEPS):
        off = lax.rem(centers[t], rows_all)
        row8 = pl.multiple_of((off // 8) * 8, 8)
        col = pl.multiple_of((off // LANES) * LANES, LANES)
        copies.append(pltpu.make_async_copy(hid.at[pl.ds(row8, 8), :], hbuf.at[t], sem.at[t, 0]))
        copies.append(pltpu.make_async_copy(val.at[:, pl.ds(col, LANES)], vbuf.at[t], sem.at[t, 1]))
        copies.append(pltpu.make_async_copy(ids.at[:, pl.ds(col, LANES)], ibuf.at[t], sem.at[t, 2]))
    for c in copies:
        c.start()
    chunks = hid.shape[1] // LANES
    rows[...] = jnp.zeros_like(rows)
    lane = lax.broadcasted_iota(jnp.int32, (K_LOC, LANES), 1)
    cols = jnp.zeros((K_LOC, LANES), F32)
    for c in copies:
        c.wait()
    for t in range(STEPS):
        off = lax.rem(centers[t], rows_all)
        blk = hbuf[t].astype(F32)
        here = lax.broadcasted_iota(jnp.int32, blk.shape, 0) == lax.rem(off, 8)
        row = jnp.sum(jnp.where(here, blk, 0.0), axis=0, keepdims=True)
        for j in range(chunks):
            rows[t * chunks + j : t * chunks + j + 1, :] = row[:, j * LANES : (j + 1) * LANES]
        here = lane == lax.rem(off, LANES)
        vcol = jnp.sum(jnp.where(here, vbuf[t].astype(F32), 0.0), axis=1, keepdims=True)
        icol = jnp.sum(jnp.where(here, ibuf[t], 0), axis=1, keepdims=True)
        parts = (
            vcol,
            (icol >> 16).astype(F32),
            ((icol >> 8) & 255).astype(F32),
            (icol & 255).astype(F32),
        )
        for q, part in enumerate(parts):
            cols = jnp.where(lane == 4 * t + q, part, cols)
    top = rows[...].astype(BF16)
    low = cols.astype(BF16)
    for d in range(out.shape[0]):
        out[d, 0:16, :] = top
        out[d, 16:32, :] = low


def square_kernel(hid, val, sq, hv, sem):
    n = sq.shape[0]
    step = hid.shape[0] // n
    copies = []
    for d in range(n):
        where = pl.ds(d * step, step)
        copies.append(pltpu.make_async_copy(hid.at[where, :], hv.at[where, :], sem.at[d]))
    for c in copies:
        c.start()
    ones = (lax.broadcasted_iota(jnp.int32, (8, hid.shape[1]), 0) == 0).astype(BF16)
    srow = lax.broadcasted_iota(jnp.int32, (8, step), 0)
    for d in range(n):
        copies[d].wait()
        h = hv[d * step : (d + 1) * step, :].astype(F32)
        s = h * h
        hi = s.astype(BF16)
        lo = (s - hi.astype(F32)).astype(BF16)
        dims = (((1,), (1,)), ((), ()))
        acc = lax.dot_general(ones, hi, dims, preferred_element_type=F32)
        acc = acc + lax.dot_general(ones, lo, dims, preferred_element_type=F32)
        v = val[:, d * step : (d + 1) * step].astype(F32)
        acc = acc + jnp.where(srow == 1, jnp.sum(v * v, axis=0, keepdims=True), 0.0)
        sq[d] = acc


def inner_kernel(centers, got, hid, val, ids, sq, out, cvec, idb, vb):
    n, _, step = sq.shape
    width = hid.shape[1]
    chunks = width // LANES
    rows_all = hid.shape[0]
    lane = lax.broadcasted_iota(jnp.int32, (K_LOC, LANES), 1)
    cvec[...] = jnp.zeros_like(cvec)
    norms = []
    for t in range(STEPS):
        owner = centers[t] // rows_all
        tile = got[owner].astype(F32)
        for j in range(chunks):
            r = t * chunks + j
            cvec[2 + t : 3 + t, j * LANES : (j + 1) * LANES] = tile[r : r + 1, :]
        low = tile[16:32, :]
        cs = [jnp.sum(jnp.where(lane == 4 * t + q, low, 0.0), axis=1, keepdims=True) for q in range(4)]
        idc = (cs[1] * 65536.0 + cs[2] * 256.0 + cs[3]).astype(jnp.int32)
        idb[t] = jnp.broadcast_to(idc, (K_LOC, LANES))
        vb[t] = jnp.broadcast_to(cs[0], (K_LOC, LANES))
        norms.append(jnp.sum(cs[0] * cs[0], axis=0, keepdims=True))
    cmat = cvec[...]
    crow = lax.broadcasted_iota(jnp.int32, (8, LANES), 0)
    tail = jnp.broadcast_to(jnp.sum(cmat * cmat, axis=1, keepdims=True), (8, LANES))
    for t in range(STEPS):
        tail = jnp.where(crow == 2 + STEPS + t, norms[t], tail)
    cb = cmat.astype(BF16)
    srow = lax.broadcasted_iota(jnp.int32, (8, step), 0)
    for d in range(n):
        part = slice(d * step, (d + 1) * step)
        acc = lax.dot_general(
            cb, hid[part, :], (((1,), (1,)), ((), ())), preferred_element_type=F32
        )
        acc = acc + sq[d]
        ident = ids[:, part]
        vals = val[:, part].astype(F32)
        for t in range(STEPS):
            w = jnp.zeros((K_LOC, step), F32)
            for l in range(K_LOC):
                idl = jnp.broadcast_to(idb[t, l : l + 1, 0:1], (K_LOC, step))
                vl = jnp.broadcast_to(vb[t, l : l + 1, 0:1], (K_LOC, step))
                w = jnp.where(ident == idl, vl, w)
            aa = jnp.sum(w * vals, axis=0, keepdims=True)
            acc = jnp.where(srow == 2 + STEPS + t, aa, acc)
        out[d, :, 0:step] = acc
        out[d, :, step:] = tail


def dist_kernel(parts, mind, sums):
    step = mind.shape[1]
    s = parts[0]
    for d in range(1, parts.shape[0]):
        s = s + parts[d]
    sq = s[0:1, 0:step] * s[1:2, 0:step]
    lane = lax.broadcasted_iota(jnp.int32, (1, LANES), 1)
    row = jnp.zeros((1, LANES), F32)
    low = None
    for t in range(STEPS):
        a, b = 2 + t, 2 + STEPS + t
        norm = s[a : a + 1, step : step + 1] * s[b : b + 1, step : step + 1]
        dist = sq + norm - 2.0 * s[a : a + 1, 0:step] * s[b : b + 1, 0:step]
        dist = jnp.maximum(dist, 0.0)
        low = dist if t == 0 else jnp.minimum(low, dist)
        row = jnp.where(lane == t, jnp.sum(low, axis=1, keepdims=True), row)
    mind[...] = low
    sums[...] = jnp.broadcast_to(row, sums.shape)


def body(hidden_states, factor_values, class_ids, centers):
    rows_all, width = hidden_states.shape
    n_dp, n_mp = lax.axis_size(DP), lax.axis_size(MP)
    n_all = n_dp * n_mp
    rows = rows_all // n_mp
    val = factor_values.T
    ids = class_ids.T
    anyspec = pl.BlockSpec(memory_space=pl.ANY)
    smem = pl.BlockSpec(memory_space=pltpu.SMEM)

    picked = pl.pallas_call(
        pick_kernel,
        out_shape=jax.ShapeDtypeStruct((n_dp, 32, LANES), BF16),
        in_specs=[smem, anyspec, anyspec, anyspec],
        out_specs=vspec(),
        scratch_shapes=[
            VMEM((STEPS, 8, width), BF16),
            VMEM((STEPS, K_LOC, LANES), BF16),
            VMEM((STEPS, K_LOC, LANES), jnp.int32),
            VMEM((16, LANES), F32),
            pltpu.SemaphoreType.DMA((STEPS, 3)),
        ],
        compiler_params=params(4),
    )(centers, hidden_states, val, ids)
    got = lax.all_to_all(picked, DP, 0, 0, tiled=True)

    sq, held = pl.pallas_call(
        square_kernel,
        out_shape=[
            jax.ShapeDtypeStruct((n_mp, 8, rows), F32),
            VMEM((rows_all, width), BF16),
        ],
        in_specs=[anyspec, vspec()],
        out_specs=[vspec(), vspec()],
        scratch_shapes=[pltpu.SemaphoreType.DMA((n_mp,))],
        compiler_params=params(24),
        cost_estimate=pl.CostEstimate(flops=8 * rows_all * width * 4, bytes_accessed=rows_all * width * 2, transcendentals=0),
    )(hidden_states, val)

    parts = pl.pallas_call(
        inner_kernel,
        out_shape=jax.ShapeDtypeStruct((n_mp, 8, rows + LANES), F32),
        in_specs=[smem] + [vspec()] * 5,
        out_specs=vspec(),
        scratch_shapes=[
            VMEM((8, width), F32),
            VMEM((STEPS, K_LOC, LANES), jnp.int32),
            VMEM((STEPS, K_LOC, LANES), F32),
        ],
        compiler_params=params(24),
    )(centers, got, held, val, ids, sq)
    parts = lax.all_to_all(parts, MP, 0, 0, tiled=True)

    mind, sums = pl.pallas_call(
        dist_kernel,
        out_shape=[
            jax.ShapeDtypeStruct((1, rows), F32),
            jax.ShapeDtypeStruct((n_all, LANES), F32),
        ],
        in_specs=[vspec()],
        out_specs=[vspec(), vspec()],
        compiler_params=params(4),
    )(parts)
    sums = lax.all_to_all(sums, DP_MP, 0, 0, tiled=True)
    means = jnp.sum(sums, axis=0)[:STEPS] / (rows_all * n_dp)
    return mind.reshape(rows), means


def solution(mesh):
    finer = Mesh(mesh.devices.reshape(2, 4, 2, 4, 2), DP_MP)
    return jax.shard_map(
        body,
        mesh=finer,
        in_specs=(P(DP, MP), P(DP, MP), P(DP, MP), P()),
        out_specs=(P(DP_MP), P()),
        check_vma=False,
    )
```

```python
import functools

import jax
import jax.numpy as jnp
from jax import lax
from jax.experimental import pallas as pl
from jax.experimental.pallas import tpu as pltpu
from jax.sharding import Mesh
from jax.sharding import PartitionSpec as P

K_LOC = 16
STEPS = 3
LANES = 128
MP = ("mp_0", "mp_1")
DP = ("dp_0", "dp_1", "dp_2")
DP_MP = ("dp_0", "dp_1", "dp_2", "mp_0", "mp_1")
VMEM = pltpu.VMEM
F32 = jnp.float32
BF16 = jnp.bfloat16


def vspec():
    return pl.BlockSpec(memory_space=VMEM)


def params(mib):
    return pltpu.CompilerParams(vmem_limit_bytes=mib * 1024 * 1024)


def pick_kernel(centers, hid, val, ids, out, cbuf, hbuf, vbuf, ibuf, rows, csem, sem):
    rows_all = hid.shape[0]
    first = pltpu.make_async_copy(centers, cbuf, csem)
    first.start()
    me = lax.axis_index(DP)
    chunks = hid.shape[1] // LANES
    rows[...] = jnp.zeros_like(rows)
    lane = lax.broadcasted_iota(jnp.int32, (K_LOC, LANES), 1)
    cols = jnp.zeros((K_LOC, LANES), F32)
    first.wait()
    copies = []
    for t in range(STEPS):
        off = lax.rem(cbuf[t], rows_all)
        row8 = pl.multiple_of((off // 8) * 8, 8)
        col = pl.multiple_of((off // LANES) * LANES, LANES)
        copies.append(pltpu.make_async_copy(hid.at[pl.ds(row8, 8), :], hbuf.at[t], sem.at[t, 0]))
        copies.append(pltpu.make_async_copy(val.at[:, pl.ds(col, LANES)], vbuf.at[t], sem.at[t, 1]))
        copies.append(pltpu.make_async_copy(ids.at[:, pl.ds(col, LANES)], ibuf.at[t], sem.at[t, 2]))
    for c in copies:
        c.start()
    for c in copies:
        c.wait()
    for t in range(STEPS):
        mine = cbuf[t] // rows_all == me
        off = jnp.where(mine, lax.rem(cbuf[t], rows_all), rows_all)
        blk = hbuf[t].astype(F32)
        srow = lax.broadcasted_iota(jnp.int32, blk.shape, 0)
        here = srow == jnp.where(mine, lax.rem(off, 8), 8)
        row = jnp.sum(jnp.where(here, blk, 0.0), axis=0, keepdims=True)
        for j in range(chunks):
            rows[t * chunks + j : t * chunks + j + 1, :] = row[:, j * LANES : (j + 1) * LANES]
        here = lane == jnp.where(mine, lax.rem(off, LANES), LANES)
        vcol = jnp.sum(jnp.where(here, vbuf[t].astype(F32), 0.0), axis=1, keepdims=True)
        icol = jnp.sum(jnp.where(here, ibuf[t], 0), axis=1, keepdims=True)
        parts = (
            vcol,
            (icol >> 16).astype(F32),
            ((icol >> 8) & 255).astype(F32),
            (icol & 255).astype(F32),
        )
        for q, part in enumerate(parts):
            cols = jnp.where(lane == 4 * t + q, part, cols)
    top = rows[...].astype(BF16)
    low = cols.astype(BF16)
    for d in range(out.shape[0]):
        out[d, 0:16, :] = top
        out[d, 16:32, :] = low


def inner_kernel(got, hid, val, ids, out, cvec, idb, vb):
    n = out.shape[0]
    step = hid.shape[0] // n
    chunks = hid.shape[1] // LANES
    lane = lax.broadcasted_iota(jnp.int32, (K_LOC, LANES), 1)
    tile = got[0].astype(F32)
    for d in range(1, got.shape[0]):
        tile = tile + got[d].astype(F32)
    low = tile[16:32, :]
    cvec[...] = jnp.zeros_like(cvec)
    norms = []
    for t in range(STEPS):
        for j in range(chunks):
            r = t * chunks + j
            cvec[2 + t : 3 + t, j * LANES : (j + 1) * LANES] = tile[r : r + 1, :]
        cs = [jnp.sum(jnp.where(lane == 4 * t + q, low, 0.0), axis=1, keepdims=True) for q in range(4)]
        idc = (cs[1] * 65536.0 + cs[2] * 256.0 + cs[3]).astype(jnp.int32)
        idb[t] = jnp.broadcast_to(idc, (K_LOC, LANES))
        vb[t] = jnp.broadcast_to(cs[0], (K_LOC, LANES))
        norms.append(jnp.sum(cs[0] * cs[0], axis=0, keepdims=True))
    cmat = cvec[...]
    crow = lax.broadcasted_iota(jnp.int32, (8, LANES), 0)
    tail = jnp.broadcast_to(jnp.sum(cmat * cmat, axis=1, keepdims=True), (8, LANES))
    for t in range(STEPS):
        tail = jnp.where(crow == 2 + STEPS + t, norms[t], tail)
    cb = cmat.astype(BF16)
    ones = (crow == 0).astype(BF16)
    srow = lax.broadcasted_iota(jnp.int32, (8, step), 0)
    dims = (((1,), (1,)), ((), ()))
    for d in range(n):
        part = slice(d * step, (d + 1) * step)
        acc = lax.dot_general(cb, hid[part, :], dims, preferred_element_type=F32)
        total = jnp.zeros((step, LANES), F32)
        for j in range(chunks):
            h = hid[part, j * LANES : (j + 1) * LANES].astype(F32)
            total = total + h * h
        hi = total.astype(BF16)
        lo = (total - hi.astype(F32)).astype(BF16)
        acc = acc + lax.dot_general(ones, hi, dims, preferred_element_type=F32)
        acc = acc + lax.dot_general(ones, lo, dims, preferred_element_type=F32)
        ident = ids[:, part]
        vals = val[:, part].astype(F32)
        acc = jnp.where(srow == 1, jnp.sum(vals * vals, axis=0, keepdims=True), acc)
        for t in range(STEPS):
            w = jnp.zeros((K_LOC, step), F32)
            for l in range(K_LOC):
                idl = jnp.broadcast_to(idb[t, l : l + 1, 0:1], (K_LOC, step))
                vl = jnp.broadcast_to(vb[t, l : l + 1, 0:1], (K_LOC, step))
                w = jnp.where(ident == idl, vl, w)
            aa = jnp.sum(w * vals, axis=0, keepdims=True)
            acc = jnp.where(srow == 2 + STEPS + t, aa, acc)
        out[d, :, 0:step] = acc
        out[d, :, step:] = tail


def dist_kernel(parts, mind, sums):
    step = mind.shape[1]
    s = parts[0]
    for d in range(1, parts.shape[0]):
        s = s + parts[d]
    sq = s[0:1, 0:step] * s[1:2, 0:step]
    lane = lax.broadcasted_iota(jnp.int32, (1, LANES), 1)
    row = jnp.zeros((1, LANES), F32)
    low = None
    for t in range(STEPS):
        a, b = 2 + t, 2 + STEPS + t
        norm = s[a : a + 1, step : step + 1] * s[b : b + 1, step : step + 1]
        dist = sq + norm - 2.0 * s[a : a + 1, 0:step] * s[b : b + 1, 0:step]
        dist = jnp.maximum(dist, 0.0)
        low = dist if t == 0 else jnp.minimum(low, dist)
        row = jnp.where(lane == t, jnp.sum(low, axis=1, keepdims=True), row)
    mind[...] = low
    sums[...] = jnp.broadcast_to(row, sums.shape)


def body(hidden_states, factor_values, class_ids, centers):
    rows_all, width = hidden_states.shape
    n_dp, n_mp = lax.axis_size(DP), lax.axis_size(MP)
    n_all = n_dp * n_mp
    rows = rows_all // n_mp
    val = factor_values.T
    ids = class_ids.T
    hbm = pl.BlockSpec(memory_space=pltpu.HBM)

    picked = pl.pallas_call(
        pick_kernel,
        out_shape=jax.ShapeDtypeStruct((n_dp, 32, LANES), BF16),
        in_specs=[hbm] * 4,
        out_specs=vspec(),
        scratch_shapes=[
            pltpu.SMEM((STEPS,), jnp.int32),
            VMEM((STEPS, 8, width), BF16),
            VMEM((STEPS, K_LOC, LANES), BF16),
            VMEM((STEPS, K_LOC, LANES), jnp.int32),
            VMEM((16, LANES), F32),
            pltpu.SemaphoreType.DMA,
            pltpu.SemaphoreType.DMA((STEPS, 3)),
        ],
        compiler_params=params(4),
    )(*(pltpu.with_memory_space_constraint(x, pltpu.HBM) for x in (centers, hidden_states, val, ids)))
    got = lax.all_to_all(picked, DP, 0, 0, tiled=True)

    parts = pl.pallas_call(
        inner_kernel,
        out_shape=jax.ShapeDtypeStruct((n_mp, 8, rows + LANES), F32),
        in_specs=[vspec()] * 4,
        out_specs=vspec(),
        scratch_shapes=[
            VMEM((8, width), F32),
            VMEM((STEPS, K_LOC, LANES), jnp.int32),
            VMEM((STEPS, K_LOC, LANES), F32),
        ],
        compiler_params=params(24),
    )(got, hidden_states, val, ids)
    parts = lax.all_to_all(parts, MP, 0, 0, tiled=True)

    mind, sums = pl.pallas_call(
        dist_kernel,
        out_shape=[
            jax.ShapeDtypeStruct((1, rows), F32),
            jax.ShapeDtypeStruct((n_all, LANES), F32),
        ],
        in_specs=[vspec()],
        out_specs=[vspec(), vspec()],
        compiler_params=params(4),
    )(parts)
    sums = lax.all_to_all(sums, DP_MP, 0, 0, tiled=True)
    means = jnp.sum(sums, axis=0)[:STEPS] / (rows_all * n_dp)
    return mind.reshape(rows), means


def solution(mesh):
    finer = Mesh(mesh.devices.reshape(2, 4, 2, 4, 2), DP_MP)
    return jax.shard_map(
        body,
        mesh=finer,
        in_specs=(P(DP, MP), P(DP, MP), P(DP, MP), P()),
        out_specs=(P(DP_MP), P()),
        check_vma=False,
    )
```

```python
import functools

import jax
import jax.numpy as jnp
from jax import lax
from jax.experimental import pallas as pl
from jax.experimental.pallas import tpu as pltpu
from jax.sharding import Mesh
from jax.sharding import PartitionSpec as P

K_LOC = 16
STEPS = 3
LANES = 128
MP = ("mp_0", "mp_1")
DP = ("dp_0", "dp_1", "dp_2")
DP_MP = ("dp_0", "dp_1", "dp_2", "mp_0", "mp_1")
VMEM = pltpu.VMEM
F32 = jnp.float32
BF16 = jnp.bfloat16


def led_by(size, first):
    return [(first + i) % size for i in range(size)]


def vspec():
    return pl.BlockSpec(memory_space=VMEM)


def params(mib):
    return pltpu.CompilerParams(vmem_limit_bytes=mib * 1024 * 1024)


def pick_kernel(centers, hid, val, ids, out, cbuf, hbuf, vbuf, ibuf, rows, csem, sem):
    rows_all = hid.shape[0]
    first = pltpu.make_async_copy(centers, cbuf, csem)
    first.start()
    me = lax.axis_index(DP)
    chunks = hid.shape[1] // LANES
    rows[...] = jnp.zeros_like(rows)
    lane = lax.broadcasted_iota(jnp.int32, (K_LOC, LANES), 1)
    cols = jnp.zeros((K_LOC, LANES), F32)
    first.wait()
    copies = []
    for t in range(STEPS):
        off = lax.rem(cbuf[t], rows_all)
        row8 = pl.multiple_of((off // 8) * 8, 8)
        col = pl.multiple_of((off // LANES) * LANES, LANES)
        copies.append(pltpu.make_async_copy(hid.at[pl.ds(row8, 8), :], hbuf.at[t], sem.at[t, 0]))
        copies.append(pltpu.make_async_copy(val.at[:, pl.ds(col, LANES)], vbuf.at[t], sem.at[t, 1]))
        copies.append(pltpu.make_async_copy(ids.at[:, pl.ds(col, LANES)], ibuf.at[t], sem.at[t, 2]))
    for c in copies:
        c.start()
    for c in copies:
        c.wait()
    for t in range(STEPS):
        mine = cbuf[t] // rows_all == me
        off = jnp.where(mine, lax.rem(cbuf[t], rows_all), rows_all)
        blk = hbuf[t].astype(F32)
        srow = lax.broadcasted_iota(jnp.int32, blk.shape, 0)
        here = srow == jnp.where(mine, lax.rem(off, 8), 8)
        row = jnp.sum(jnp.where(here, blk, 0.0), axis=0, keepdims=True)
        for j in range(chunks):
            rows[t * chunks + j : t * chunks + j + 1, :] = row[:, j * LANES : (j + 1) * LANES]
        here = lane == jnp.where(mine, lax.rem(off, LANES), LANES)
        vcol = jnp.sum(jnp.where(here, vbuf[t].astype(F32), 0.0), axis=1, keepdims=True)
        icol = jnp.sum(jnp.where(here, ibuf[t], 0), axis=1, keepdims=True)
        parts = (
            vcol,
            (icol >> 16).astype(F32),
            ((icol >> 8) & 255).astype(F32),
            (icol & 255).astype(F32),
        )
        for q, part in enumerate(parts):
            cols = jnp.where(lane == 4 * t + q, part, cols)
    top = rows[...].astype(BF16)
    low = cols.astype(BF16)
    for d in range(out.shape[0]):
        out[d, 0:16, :] = top
        out[d, 16:32, :] = low


def inner_kernel(first, got, hid, val, ids, out, cvec, idb, vb):
    n = out.shape[0]
    step = hid.shape[0] // n
    chunks = hid.shape[1] // LANES
    lane = lax.broadcasted_iota(jnp.int32, (K_LOC, LANES), 1)
    tile = got[0].astype(F32)
    for d in range(1, got.shape[0]):
        tile = tile + got[d].astype(F32)
    low = tile[16:32, :]
    cvec[...] = jnp.zeros_like(cvec)
    norms = []
    for t in range(STEPS):
        for j in range(chunks):
            r = t * chunks + j
            cvec[2 + t : 3 + t, j * LANES : (j + 1) * LANES] = tile[r : r + 1, :]
        cs = [jnp.sum(jnp.where(lane == 4 * t + q, low, 0.0), axis=1, keepdims=True) for q in range(4)]
        idc = (cs[1] * 65536.0 + cs[2] * 256.0 + cs[3]).astype(jnp.int32)
        idb[t] = jnp.broadcast_to(idc, (K_LOC, LANES))
        vb[t] = jnp.broadcast_to(cs[0], (K_LOC, LANES))
        norms.append(jnp.sum(cs[0] * cs[0], axis=0, keepdims=True))
    cmat = cvec[...]
    crow = lax.broadcasted_iota(jnp.int32, (8, LANES), 0)
    tail = jnp.broadcast_to(jnp.sum(cmat * cmat, axis=1, keepdims=True), (8, LANES))
    for t in range(STEPS):
        tail = jnp.where(crow == 2 + STEPS + t, norms[t], tail)
    cb = cmat.astype(BF16)
    ones = (crow == 0).astype(BF16)
    srow = lax.broadcasted_iota(jnp.int32, (8, step), 0)
    dims = (((1,), (1,)), ((), ()))
    for d in range(n):
        part = slice(d * step, (d + 1) * step)
        acc = lax.dot_general(cb, hid[part, :], dims, preferred_element_type=F32)
        total = jnp.zeros((step, LANES), F32)
        for j in range(chunks):
            h = hid[part, j * LANES : (j + 1) * LANES].astype(F32)
            total = total + h * h
        hi = total.astype(BF16)
        lo = (total - hi.astype(F32)).astype(BF16)
        acc = acc + lax.dot_general(ones, hi, dims, preferred_element_type=F32)
        acc = acc + lax.dot_general(ones, lo, dims, preferred_element_type=F32)
        ident = ids[:, part]
        vals = val[:, part].astype(F32)
        acc = jnp.where(srow == 1, jnp.sum(vals * vals, axis=0, keepdims=True), acc)
        for t in range(STEPS):
            w = jnp.zeros((K_LOC, step), F32)
            for l in range(K_LOC):
                idl = jnp.broadcast_to(idb[t, l : l + 1, 0:1], (K_LOC, step))
                vl = jnp.broadcast_to(vb[t, l : l + 1, 0:1], (K_LOC, step))
                w = jnp.where(ident == idl, vl, w)
            aa = jnp.sum(w * vals, axis=0, keepdims=True)
            acc = jnp.where(srow == 2 + STEPS + t, aa, acc)
        slot = (d - first) % n
        out[slot, :, 0:step] = acc
        out[slot, :, step:] = tail


def dist_kernel(parts, mind, sums):
    step = mind.shape[1]
    s = parts[0]
    for d in range(1, parts.shape[0]):
        s = s + parts[d]
    sq = s[0:1, 0:step] * s[1:2, 0:step]
    lane = lax.broadcasted_iota(jnp.int32, (1, LANES), 1)
    row = jnp.zeros((1, LANES), F32)
    low = None
    for t in range(STEPS):
        a, b = 2 + t, 2 + STEPS + t
        norm = s[a : a + 1, step : step + 1] * s[b : b + 1, step : step + 1]
        dist = sq + norm - 2.0 * s[a : a + 1, 0:step] * s[b : b + 1, 0:step]
        dist = jnp.maximum(dist, 0.0)
        low = dist if t == 0 else jnp.minimum(low, dist)
        row = jnp.where(lane == t, jnp.sum(low, axis=1, keepdims=True), row)
    mind[...] = low
    sums[...] = jnp.broadcast_to(row, sums.shape)


def body(hidden_states, factor_values, class_ids, centers):
    rows_all, width = hidden_states.shape
    n_dp, n_mp = lax.axis_size(DP), lax.axis_size(MP)
    n_all = n_dp * n_mp
    rows = rows_all // n_mp
    val = factor_values.T
    ids = class_ids.T
    first = 3 * n_mp // 4
    hbm = pl.BlockSpec(memory_space=pltpu.HBM)

    picked = pl.pallas_call(
        pick_kernel,
        out_shape=jax.ShapeDtypeStruct((n_dp, 32, LANES), BF16),
        in_specs=[hbm] * 4,
        out_specs=vspec(),
        scratch_shapes=[
            pltpu.SMEM((STEPS,), jnp.int32),
            VMEM((STEPS, 8, width), BF16),
            VMEM((STEPS, K_LOC, LANES), BF16),
            VMEM((STEPS, K_LOC, LANES), jnp.int32),
            VMEM((16, LANES), F32),
            pltpu.SemaphoreType.DMA,
            pltpu.SemaphoreType.DMA((STEPS, 3)),
        ],
        compiler_params=params(4),
    )(*(pltpu.with_memory_space_constraint(x, pltpu.HBM) for x in (centers, hidden_states, val, ids)))
    got = lax.all_to_all(picked, DP, 0, 0, tiled=True, axis_index_groups=[led_by(n_dp, 3 * n_dp // 4)])

    parts = pl.pallas_call(
        functools.partial(inner_kernel, first),
        out_shape=jax.ShapeDtypeStruct((n_mp, 8, rows + LANES), F32),
        in_specs=[vspec()] * 4,
        out_specs=vspec(),
        scratch_shapes=[
            VMEM((8, width), F32),
            VMEM((STEPS, K_LOC, LANES), jnp.int32),
            VMEM((STEPS, K_LOC, LANES), F32),
        ],
        compiler_params=params(24),
    )(got, hidden_states, val, ids)
    parts = lax.all_to_all(parts, MP, 0, 0, tiled=True, axis_index_groups=[led_by(n_mp, first)])

    mind, sums = pl.pallas_call(
        dist_kernel,
        out_shape=[
            jax.ShapeDtypeStruct((1, rows), F32),
            jax.ShapeDtypeStruct((n_all, LANES), F32),
        ],
        in_specs=[vspec()],
        out_specs=[vspec(), vspec()],
        compiler_params=params(4),
    )(parts)
    sums = lax.all_to_all(sums, DP_MP, 0, 0, tiled=True)
    means = jnp.sum(sums, axis=0)[:STEPS] / (rows_all * n_dp)
    return mind.reshape(rows), means


def solution(mesh):
    finer = Mesh(mesh.devices.reshape(2, 4, 2, 4, 2), DP_MP)
    return jax.shard_map(
        body,
        mesh=finer,
        in_specs=(P(DP, MP), P(DP, MP), P(DP, MP), P()),
        out_specs=(P(DP_MP), P()),
        check_vma=False,
    )
```

```python
import functools

import jax
import jax.numpy as jnp
from jax import lax
from jax.experimental import pallas as pl
from jax.experimental.pallas import tpu as pltpu
from jax.sharding import Mesh
from jax.sharding import PartitionSpec as P

K_LOC = 16
STEPS = 3
LANES = 128
MP = ("mp_0", "mp_1")
DP = ("dp_0", "dp_1", "dp_2")
DP_MP = ("dp_0", "dp_1", "dp_2", "mp_0", "mp_1")
VMEM = pltpu.VMEM
F32 = jnp.float32
BF16 = jnp.bfloat16


def led_by(size, first):
    return [(first + i) % size for i in range(size)]


def vspec():
    return pl.BlockSpec(memory_space=VMEM)


def params(mib):
    return pltpu.CompilerParams(vmem_limit_bytes=mib * 1024 * 1024)


def pick_kernel(centers, hid, val, ids, out, cbuf, hbuf, vbuf, ibuf, rows, csem, sem):
    rows_all = hid.shape[0]
    first = pltpu.make_async_copy(centers, cbuf, csem)
    first.start()
    me = lax.axis_index(DP)
    chunks = hid.shape[1] // LANES
    out[...] = jnp.zeros_like(out)
    rows[...] = jnp.zeros_like(rows)
    lane = lax.broadcasted_iota(jnp.int32, (K_LOC, LANES), 1)
    first.wait()
    mine = [cbuf[t] // rows_all == me for t in range(STEPS)]

    @pl.when(functools.reduce(jnp.logical_or, mine))
    def _():
        copies = []
        for t in range(STEPS):
            off = lax.rem(cbuf[t], rows_all)
            row8 = pl.multiple_of((off // 8) * 8, 8)
            col = pl.multiple_of((off // LANES) * LANES, LANES)
            copies.append(pltpu.make_async_copy(hid.at[pl.ds(row8, 8), :], hbuf.at[t], sem.at[t, 0]))
            copies.append(pltpu.make_async_copy(val.at[:, pl.ds(col, LANES)], vbuf.at[t], sem.at[t, 1]))
            copies.append(pltpu.make_async_copy(ids.at[:, pl.ds(col, LANES)], ibuf.at[t], sem.at[t, 2]))
        for c in copies:
            c.start()
        for c in copies:
            c.wait()
        cols = jnp.zeros((K_LOC, LANES), F32)
        for t in range(STEPS):
            off = lax.rem(cbuf[t], rows_all)
            blk = hbuf[t].astype(F32)
            srow = lax.broadcasted_iota(jnp.int32, blk.shape, 0)
            here = srow == jnp.where(mine[t], lax.rem(off, 8), 8)
            row = jnp.sum(jnp.where(here, blk, 0.0), axis=0, keepdims=True)
            for j in range(chunks):
                rows[t * chunks + j : t * chunks + j + 1, :] = row[:, j * LANES : (j + 1) * LANES]
            here = lane == jnp.where(mine[t], lax.rem(off, LANES), LANES)
            vcol = jnp.sum(jnp.where(here, vbuf[t].astype(F32), 0.0), axis=1, keepdims=True)
            icol = jnp.sum(jnp.where(here, ibuf[t], 0), axis=1, keepdims=True)
            parts = (
                vcol,
                (icol >> 16).astype(F32),
                ((icol >> 8) & 255).astype(F32),
                (icol & 255).astype(F32),
            )
            for q, part in enumerate(parts):
                cols = jnp.where(lane == 4 * t + q, part, cols)
        top = rows[...].astype(BF16)
        low = cols.astype(BF16)
        for d in range(out.shape[0]):
            out[d, 0:16, :] = top
            out[d, 16:32, :] = low


def inner_kernel(first, got, hid, val, ids, out, cvec, idb, vb):
    n = out.shape[0]
    step = hid.shape[0] // n
    chunks = hid.shape[1] // LANES
    lane = lax.broadcasted_iota(jnp.int32, (K_LOC, LANES), 1)
    tile = got[0].astype(F32)
    for d in range(1, got.shape[0]):
        tile = tile + got[d].astype(F32)
    low = tile[16:32, :]
    cvec[...] = jnp.zeros_like(cvec)
    norms = []
    for t in range(STEPS):
        for j in range(chunks):
            r = t * chunks + j
            cvec[2 + t : 3 + t, j * LANES : (j + 1) * LANES] = tile[r : r + 1, :]
        cs = [jnp.sum(jnp.where(lane == 4 * t + q, low, 0.0), axis=1, keepdims=True) for q in range(4)]
        idc = (cs[1] * 65536.0 + cs[2] * 256.0 + cs[3]).astype(jnp.int32)
        for l in range(K_LOC):
            idb[t * K_LOC + l] = jnp.broadcast_to(idc[l : l + 1, :], (K_LOC, LANES)).astype(jnp.int16)
            vb[t * K_LOC + l] = jnp.broadcast_to(cs[0][l : l + 1, :], (K_LOC, LANES)).astype(BF16)
        norms.append(jnp.sum(cs[0] * cs[0], axis=0, keepdims=True))
    cmat = cvec[...]
    crow = lax.broadcasted_iota(jnp.int32, (8, LANES), 0)
    tail = jnp.broadcast_to(jnp.sum(cmat * cmat, axis=1, keepdims=True), (8, LANES))
    for t in range(STEPS):
        tail = jnp.where(crow == 2 + STEPS + t, norms[t], tail)
    cb = cmat.astype(BF16)
    ones = (crow == 0).astype(BF16)
    srow = lax.broadcasted_iota(jnp.int32, (8, step), 0)
    dims = (((1,), (1,)), ((), ()))
    tiles = step // LANES
    for d in range(n):
        part = slice(d * step, (d + 1) * step)
        acc = lax.dot_general(cb, hid[part, :], dims, preferred_element_type=F32)
        total = None
        for j in range(chunks):
            h = hid[part, j * LANES : (j + 1) * LANES].astype(F32)
            total = h * h if total is None else total + h * h
        hi = total.astype(BF16)
        lo = (total - hi.astype(F32)).astype(BF16)
        acc = acc + lax.dot_general(ones, hi, dims, preferred_element_type=F32)
        acc = acc + lax.dot_general(ones, lo, dims, preferred_element_type=F32)
        ident = ids[:, part].astype(jnp.int16)
        vals = val[:, part].astype(F32)
        acc = jnp.where(srow == 1, jnp.sum(vals * vals, axis=0, keepdims=True), acc)
        for t in range(STEPS):
            w = [jnp.zeros((K_LOC, LANES), BF16)] * tiles
            for l in range(K_LOC):
                idl = idb[t * K_LOC + l]
                vl = vb[t * K_LOC + l]
                w = [jnp.where(ident[:, k * LANES : (k + 1) * LANES] == idl, vl, w[k]) for k in range(tiles)]
            w = jnp.concatenate(w, axis=1)
            aa = jnp.sum(w.astype(F32) * vals, axis=0, keepdims=True)
            acc = jnp.where(srow == 2 + STEPS + t, aa, acc)
        slot = (d - first) % n
        out[slot, :, 0:step] = acc
        out[slot, :, step:] = tail


def dist_kernel(parts, mind, sums):
    step = mind.shape[1]
    s = parts[0]
    for d in range(1, parts.shape[0]):
        s = s + parts[d]
    sq = s[0:1, 0:step] * s[1:2, 0:step]
    lane = lax.broadcasted_iota(jnp.int32, (1, LANES), 1)
    row = jnp.zeros((1, LANES), F32)
    low = None
    for t in range(STEPS):
        a, b = 2 + t, 2 + STEPS + t
        norm = s[a : a + 1, step : step + 1] * s[b : b + 1, step : step + 1]
        dist = sq + norm - 2.0 * s[a : a + 1, 0:step] * s[b : b + 1, 0:step]
        dist = jnp.maximum(dist, 0.0)
        low = dist if t == 0 else jnp.minimum(low, dist)
        row = jnp.where(lane == t, jnp.sum(low, axis=1, keepdims=True), row)
    mind[...] = low
    sums[...] = jnp.broadcast_to(row, sums.shape)


def mean_kernel(pool, sums, mind, out, low):
    low[...] = mind[...]
    total = jnp.sum(sums[...], axis=0) / pool
    out[...] = total[0 : out.shape[0]]


def body(hidden_states, factor_values, class_ids, centers):
    rows_all, width = hidden_states.shape
    n_dp, n_mp = lax.axis_size(DP), lax.axis_size(MP)
    n_all = n_dp * n_mp
    rows = rows_all // n_mp
    val = factor_values.T
    ids = class_ids.T
    first = 3 * n_mp // 4
    hbm = pl.BlockSpec(memory_space=pltpu.HBM)

    picked = pl.pallas_call(
        pick_kernel,
        out_shape=jax.ShapeDtypeStruct((n_dp, 32, LANES), BF16),
        in_specs=[hbm] * 4,
        out_specs=vspec(),
        scratch_shapes=[
            pltpu.SMEM((STEPS,), jnp.int32),
            VMEM((STEPS, 8, width), BF16),
            VMEM((STEPS, K_LOC, LANES), BF16),
            VMEM((STEPS, K_LOC, LANES), jnp.int32),
            VMEM((16, LANES), F32),
            pltpu.SemaphoreType.DMA,
            pltpu.SemaphoreType.DMA((STEPS, 3)),
        ],
        compiler_params=params(4),
    )(*(pltpu.with_memory_space_constraint(x, pltpu.HBM) for x in (centers, hidden_states, val, ids)))
    got = lax.all_to_all(picked, DP, 0, 0, tiled=True, axis_index_groups=[led_by(n_dp, 3 * n_dp // 4)])

    parts = pl.pallas_call(
        functools.partial(inner_kernel, first),
        out_shape=jax.ShapeDtypeStruct((n_mp, 8, rows + LANES), F32),
        in_specs=[vspec()] * 4,
        out_specs=vspec(),
        scratch_shapes=[
            VMEM((8, width), F32),
            VMEM((STEPS * K_LOC, K_LOC, LANES), jnp.int16),
            VMEM((STEPS * K_LOC, K_LOC, LANES), BF16),
        ],
        compiler_params=params(24),
    )(got, hidden_states, val, ids)
    parts = lax.all_to_all(parts, MP, 0, 0, tiled=True, axis_index_groups=[led_by(n_mp, first)])

    mind, sums = pl.pallas_call(
        dist_kernel,
        out_shape=[
            VMEM((1, rows), F32),
            jax.ShapeDtypeStruct((n_all, LANES), F32),
        ],
        in_specs=[vspec()],
        out_specs=[vspec(), vspec()],
        compiler_params=params(4),
    )(parts)
    sums = lax.all_to_all(sums, DP_MP, 0, 0, tiled=True)
    means, mind = pl.pallas_call(
        functools.partial(mean_kernel, rows_all * n_dp),
        out_shape=[jax.ShapeDtypeStruct((STEPS,), F32), jax.ShapeDtypeStruct((1, rows), F32)],
        in_specs=[vspec(), vspec()],
        out_specs=[vspec(), vspec()],
        compiler_params=params(4),
    )(sums, mind)
    return mind.reshape(rows), means


def solution(mesh):
    finer = Mesh(mesh.devices.reshape(2, 4, 2, 4, 2), DP_MP)
    return jax.shard_map(
        body,
        mesh=finer,
        in_specs=(P(DP, MP), P(DP, MP), P(DP, MP), P()),
        out_specs=(P(DP_MP), P()),
        check_vma=False,
    )
```

```python
import functools

import jax
import jax.numpy as jnp
from jax import lax
from jax.experimental import pallas as pl
from jax.experimental.pallas import tpu as pltpu
from jax.sharding import Mesh
from jax.sharding import PartitionSpec as P

K_LOC = 16
STEPS = 3
LANES = 128
MP = ("mp_0", "mp_1")
DP = ("dp_0", "dp_1", "dp_2")
DP_MP = ("dp_0", "dp_1", "dp_2", "mp_0", "mp_1")
VMEM = pltpu.VMEM
F32 = jnp.float32
BF16 = jnp.bfloat16


def led_by(size, first):
    return [(first + i) % size for i in range(size)]


def vspec():
    return pl.BlockSpec(memory_space=VMEM)


def params(mib):
    return pltpu.CompilerParams(vmem_limit_bytes=mib * 1024 * 1024)


def pick_kernel(centers, hid, val, ids, out, cbuf, hbuf, vbuf, ibuf, rows, csem, sem):
    rows_all = hid.shape[0]
    first = pltpu.make_async_copy(centers, cbuf, csem)
    first.start()
    me = lax.axis_index(DP)
    chunks = hid.shape[1] // LANES
    out[...] = jnp.zeros_like(out)
    rows[...] = jnp.zeros_like(rows)
    lane = lax.broadcasted_iota(jnp.int32, (K_LOC, LANES), 1)
    first.wait()
    mine = [cbuf[t] // rows_all == me for t in range(STEPS)]

    @pl.when(functools.reduce(jnp.logical_or, mine))
    def _():
        copies = []
        for t in range(STEPS):
            off = lax.rem(cbuf[t], rows_all)
            row8 = pl.multiple_of((off // 8) * 8, 8)
            col = pl.multiple_of((off // LANES) * LANES, LANES)
            copies.append(pltpu.make_async_copy(hid.at[pl.ds(row8, 8), :], hbuf.at[t], sem.at[t, 0]))
            copies.append(pltpu.make_async_copy(val.at[:, pl.ds(col, LANES)], vbuf.at[t], sem.at[t, 1]))
            copies.append(pltpu.make_async_copy(ids.at[:, pl.ds(col, LANES)], ibuf.at[t], sem.at[t, 2]))
        for c in copies:
            c.start()
        for c in copies:
            c.wait()
        cols = jnp.zeros((K_LOC, LANES), F32)
        for t in range(STEPS):
            off = lax.rem(cbuf[t], rows_all)
            blk = hbuf[t].astype(F32)
            srow = lax.broadcasted_iota(jnp.int32, blk.shape, 0)
            here = srow == jnp.where(mine[t], lax.rem(off, 8), 8)
            row = jnp.sum(jnp.where(here, blk, 0.0), axis=0, keepdims=True)
            for j in range(chunks):
                rows[t * chunks + j : t * chunks + j + 1, :] = row[:, j * LANES : (j + 1) * LANES]
            here = lane == jnp.where(mine[t], lax.rem(off, LANES), LANES)
            vcol = jnp.sum(jnp.where(here, vbuf[t].astype(F32), 0.0), axis=1, keepdims=True)
            icol = jnp.sum(jnp.where(here, ibuf[t], 0), axis=1, keepdims=True)
            parts = (
                vcol,
                (icol >> 16).astype(F32),
                ((icol >> 8) & 255).astype(F32),
                (icol & 255).astype(F32),
            )
            for q, part in enumerate(parts):
                cols = jnp.where(lane == 4 * t + q, part, cols)
        top = rows[...].astype(BF16)
        low = cols.astype(BF16)
        for d in range(out.shape[0]):
            out[d, 0:16, :] = top
            out[d, 16:32, :] = low


def inner_kernel(first, got, hid, val, ids, out, cvec, idb, vb):
    n = out.shape[0]
    step = hid.shape[0] // n
    chunks = hid.shape[1] // LANES
    lane = lax.broadcasted_iota(jnp.int32, (K_LOC, LANES), 1)
    tile = got[0].astype(F32)
    for d in range(1, got.shape[0]):
        tile = tile + got[d].astype(F32)
    low = tile[16:32, :]
    cvec[...] = jnp.zeros_like(cvec)
    norms = []
    for t in range(STEPS):
        for j in range(chunks):
            r = t * chunks + j
            cvec[2 + t : 3 + t, j * LANES : (j + 1) * LANES] = tile[r : r + 1, :]
        cs = [jnp.sum(jnp.where(lane == 4 * t + q, low, 0.0), axis=1, keepdims=True) for q in range(4)]
        idc = (cs[1] * 65536.0 + cs[2] * 256.0 + cs[3]).astype(jnp.int32)
        for l in range(K_LOC):
            idb[t * K_LOC + l] = jnp.broadcast_to(idc[l : l + 1, :], (K_LOC, LANES)).astype(jnp.int16)
            vb[t * K_LOC + l] = jnp.broadcast_to(cs[0][l : l + 1, :], (K_LOC, LANES)).astype(BF16)
        norms.append(jnp.sum(cs[0] * cs[0], axis=0, keepdims=True))
    cmat = cvec[...]
    crow = lax.broadcasted_iota(jnp.int32, (8, LANES), 0)
    tail = jnp.broadcast_to(jnp.sum(cmat * cmat, axis=1, keepdims=True), (8, LANES))
    for t in range(STEPS):
        tail = jnp.where(crow == 2 + STEPS + t, norms[t], tail)
    cb = cmat.astype(BF16)
    ones = (crow == 0).astype(BF16)
    srow = lax.broadcasted_iota(jnp.int32, (8, step), 0)
    dims = (((1,), (1,)), ((), ()))
    tiles = step // LANES
    for d in range(n):
        part = slice(d * step, (d + 1) * step)
        acc = lax.dot_general(cb, hid[part, :], dims, preferred_element_type=F32)
        total = None
        for j in range(chunks):
            h = hid[part, j * LANES : (j + 1) * LANES].astype(F32)
            total = h * h if total is None else total + h * h
        hi = total.astype(BF16)
        lo = (total - hi.astype(F32)).astype(BF16)
        acc = acc + lax.dot_general(ones, hi, dims, preferred_element_type=F32)
        acc = acc + lax.dot_general(ones, lo, dims, preferred_element_type=F32)
        ident = ids[:, part].astype(jnp.int16)
        vals = val[:, part].astype(F32)
        acc = jnp.where(srow == 1, jnp.sum(vals * vals, axis=0, keepdims=True), acc)
        for t in range(STEPS):
            w = [jnp.zeros((K_LOC, LANES), BF16)] * tiles
            for l in range(K_LOC):
                idl = idb[t * K_LOC + l]
                vl = vb[t * K_LOC + l]
                w = [jnp.where(ident[:, k * LANES : (k + 1) * LANES] == idl, vl, w[k]) for k in range(tiles)]
            w = jnp.concatenate(w, axis=1)
            aa = jnp.sum(w.astype(F32) * vals, axis=0, keepdims=True)
            acc = jnp.where(srow == 2 + STEPS + t, aa, acc)
        slot = (d - first) % n
        out[slot, :, 0:step] = acc
        out[slot, :, step:] = tail


def dist_kernel(parts, mind, sums):
    step = mind.shape[1]
    s = parts[0]
    for d in range(1, parts.shape[0]):
        s = s + parts[d]
    sq = s[0:1, 0:step] * s[1:2, 0:step]
    lane = lax.broadcasted_iota(jnp.int32, (1, LANES), 1)
    row = jnp.zeros((1, LANES), F32)
    low = None
    for t in range(STEPS):
        a, b = 2 + t, 2 + STEPS + t
        norm = s[a : a + 1, step : step + 1] * s[b : b + 1, step : step + 1]
        dist = sq + norm - 2.0 * s[a : a + 1, 0:step] * s[b : b + 1, 0:step]
        dist = jnp.maximum(dist, 0.0)
        low = dist if t == 0 else jnp.minimum(low, dist)
        row = jnp.where(lane == t, jnp.sum(low, axis=1, keepdims=True), row)
    mind[...] = low
    sums[...] = jnp.broadcast_to(row, sums.shape)


def pair_kernel(own, other, sums):
    sums[...] = jnp.broadcast_to(own[0:1, :] + other[0:1, :], sums.shape)


def mean_kernel(pool, sums, mind, out, low):
    low[...] = mind[...]
    total = jnp.sum(sums[...], axis=0) / pool
    out[...] = total[0 : out.shape[0]]


def body(hidden_states, factor_values, class_ids, centers):
    rows_all, width = hidden_states.shape
    n_dp, n_mp = lax.axis_size(DP), lax.axis_size(MP)
    n_all = n_dp * n_mp
    rows = rows_all // n_mp
    val = factor_values.T
    ids = class_ids.T
    first = 6
    hbm = pl.BlockSpec(memory_space=pltpu.HBM)

    picked = pl.pallas_call(
        pick_kernel,
        out_shape=jax.ShapeDtypeStruct((n_dp, 32, LANES), BF16),
        in_specs=[hbm] * 4,
        out_specs=vspec(),
        scratch_shapes=[
            pltpu.SMEM((STEPS,), jnp.int32),
            VMEM((STEPS, 8, width), BF16),
            VMEM((STEPS, K_LOC, LANES), BF16),
            VMEM((STEPS, K_LOC, LANES), jnp.int32),
            VMEM((16, LANES), F32),
            pltpu.SemaphoreType.DMA,
            pltpu.SemaphoreType.DMA((STEPS, 3)),
        ],
        compiler_params=params(4),
    )(*(pltpu.with_memory_space_constraint(x, pltpu.HBM) for x in (centers, hidden_states, val, ids)))
    got = lax.all_to_all(picked, DP, 0, 0, tiled=True, axis_index_groups=[led_by(n_dp, 13)])

    parts = pl.pallas_call(
        functools.partial(inner_kernel, first),
        out_shape=jax.ShapeDtypeStruct((n_mp, 8, rows + LANES), F32),
        in_specs=[vspec()] * 4,
        out_specs=vspec(),
        scratch_shapes=[
            VMEM((8, width), F32),
            VMEM((STEPS * K_LOC, K_LOC, LANES), jnp.int16),
            VMEM((STEPS * K_LOC, K_LOC, LANES), BF16),
        ],
        compiler_params=params(24),
    )(got, hidden_states, val, ids)
    parts = lax.all_to_all(parts, MP, 0, 0, tiled=True, axis_index_groups=[led_by(n_mp, first)])

    mind, sums = pl.pallas_call(
        dist_kernel,
        out_shape=[
            VMEM((1, rows), F32),
            jax.ShapeDtypeStruct((8, LANES), F32),
        ],
        in_specs=[vspec()],
        out_specs=[vspec(), vspec()],
        compiler_params=params(4),
    )(parts)
    other = lax.ppermute(sums, "dp_2", [(0, 1), (1, 0)])
    sums = pl.pallas_call(
        pair_kernel,
        out_shape=jax.ShapeDtypeStruct((n_all // 2, LANES), F32),
        in_specs=[vspec(), vspec()],
        out_specs=vspec(),
        compiler_params=params(4),
    )(sums, other)
    sums = lax.all_to_all(sums, ("dp_0", "dp_1", "mp_0", "mp_1"), 0, 0, tiled=True, axis_index_groups=[led_by(n_all // 2, 54)])
    means, mind = pl.pallas_call(
        functools.partial(mean_kernel, rows_all * n_dp),
        out_shape=[jax.ShapeDtypeStruct((STEPS,), F32), jax.ShapeDtypeStruct((1, rows), F32)],
        in_specs=[vspec(), vspec()],
        out_specs=[vspec(), vspec()],
        compiler_params=params(4),
    )(sums, mind)
    return mind.reshape(rows), means


def solution(mesh):
    finer = Mesh(mesh.devices.reshape(2, 4, 2, 4, 2), DP_MP)
    return jax.shard_map(
        body,
        mesh=finer,
        in_specs=(P(DP, MP), P(DP, MP), P(DP, MP), P()),
        out_specs=(P(DP_MP), P()),
        check_vma=False,
    )
```

```python
import functools

import jax
import jax.numpy as jnp
from jax import lax
from jax.experimental import pallas as pl
from jax.experimental.pallas import tpu as pltpu
from jax.sharding import Mesh
from jax.sharding import PartitionSpec as P

K_LOC = 16
STEPS = 3
LANES = 128
MP = ("mp_0", "mp_1")
DP = ("dp_0", "dp_1", "dp_2")
DP_MP = ("dp_0", "dp_1", "dp_2", "mp_0", "mp_1")
VMEM = pltpu.VMEM
F32 = jnp.float32
BF16 = jnp.bfloat16


def led_by(size, first):
    return [(first + i) % size for i in range(size)]


def vspec():
    return pl.BlockSpec(memory_space=VMEM)


def params(mib):
    return pltpu.CompilerParams(vmem_limit_bytes=mib * 1024 * 1024)


def pick_kernel(centers, hid, val, ids, out, cbuf, hbuf, vbuf, ibuf, rows, csem, sem):
    rows_all = hid.shape[0]
    first = pltpu.make_async_copy(centers, cbuf, csem)
    first.start()
    me = lax.axis_index(DP)
    chunks = hid.shape[1] // LANES
    out[...] = jnp.zeros_like(out)
    rows[...] = jnp.zeros_like(rows)
    lane = lax.broadcasted_iota(jnp.int32, (K_LOC, LANES), 1)
    first.wait()
    mine = [cbuf[t] // rows_all == me for t in range(STEPS)]

    @pl.when(functools.reduce(jnp.logical_or, mine))
    def _():
        copies = []
        for t in range(STEPS):
            off = lax.rem(cbuf[t], rows_all)
            row8 = pl.multiple_of((off // 8) * 8, 8)
            col = pl.multiple_of((off // LANES) * LANES, LANES)
            copies.append(pltpu.make_async_copy(hid.at[pl.ds(row8, 8), :], hbuf.at[t], sem.at[t, 0]))
            copies.append(pltpu.make_async_copy(val.at[:, pl.ds(col, LANES)], vbuf.at[t], sem.at[t, 1]))
            copies.append(pltpu.make_async_copy(ids.at[:, pl.ds(col, LANES)], ibuf.at[t], sem.at[t, 2]))
        for c in copies:
            c.start()
        for c in copies:
            c.wait()
        cols = jnp.zeros((K_LOC, LANES), F32)
        for t in range(STEPS):
            off = lax.rem(cbuf[t], rows_all)
            blk = hbuf[t].astype(F32)
            srow = lax.broadcasted_iota(jnp.int32, blk.shape, 0)
            here = srow == jnp.where(mine[t], lax.rem(off, 8), 8)
            row = jnp.sum(jnp.where(here, blk, 0.0), axis=0, keepdims=True)
            for j in range(chunks):
                rows[t * chunks + j : t * chunks + j + 1, :] = row[:, j * LANES : (j + 1) * LANES]
            here = lane == jnp.where(mine[t], lax.rem(off, LANES), LANES)
            vcol = jnp.sum(jnp.where(here, vbuf[t].astype(F32), 0.0), axis=1, keepdims=True)
            icol = jnp.sum(jnp.where(here, ibuf[t], 0), axis=1, keepdims=True)
            parts = (
                vcol,
                (icol >> 16).astype(F32),
                ((icol >> 8) & 255).astype(F32),
                (icol & 255).astype(F32),
            )
            for q, part in enumerate(parts):
                cols = jnp.where(lane == 4 * t + q, part, cols)
        top = rows[...].astype(BF16)
        low = cols.astype(BF16)
        for d in range(out.shape[0]):
            out[d, 0:16, :] = top
            out[d, 16:32, :] = low


def inner_kernel(first, got, hid, val, ids, out, cvec, idb, vb):
    n = out.shape[0]
    step = hid.shape[0] // n
    chunks = hid.shape[1] // LANES
    lane = lax.broadcasted_iota(jnp.int32, (K_LOC, LANES), 1)
    tile = got[0].astype(F32)
    for d in range(1, got.shape[0]):
        tile = tile + got[d].astype(F32)
    low = tile[16:32, :]
    cvec[...] = jnp.zeros_like(cvec)
    norms = []
    for t in range(STEPS):
        for j in range(chunks):
            r = t * chunks + j
            cvec[2 + t : 3 + t, j * LANES : (j + 1) * LANES] = tile[r : r + 1, :]
        cs = [jnp.sum(jnp.where(lane == 4 * t + q, low, 0.0), axis=1, keepdims=True) for q in range(4)]
        idc = (cs[1] * 65536.0 + cs[2] * 256.0 + cs[3]).astype(jnp.int32)
        for l in range(K_LOC):
            idb[t * K_LOC + l] = jnp.broadcast_to(idc[l : l + 1, :], (K_LOC, LANES)).astype(jnp.int16)
            vb[t * K_LOC + l] = jnp.broadcast_to(cs[0][l : l + 1, :], (K_LOC, LANES)).astype(BF16)
        norms.append(jnp.sum(cs[0] * cs[0], axis=0, keepdims=True))
    cmat = cvec[...]
    crow = lax.broadcasted_iota(jnp.int32, (8, LANES), 0)
    tail = jnp.broadcast_to(jnp.sum(cmat * cmat, axis=1, keepdims=True), (8, LANES))
    for t in range(STEPS):
        tail = jnp.where(crow == 2 + STEPS + t, norms[t], tail)
    cb = cmat.astype(BF16)
    srow = lax.broadcasted_iota(jnp.int32, (8, step), 0)
    dims = (((1,), (1,)), ((), ()))
    tiles = step // LANES
    for d in range(n):
        part = slice(d * step, (d + 1) * step)
        acc = lax.dot_general(cb, hid[part, :], dims, preferred_element_type=F32)
        total = None
        for j in range(chunks):
            h = hid[part, j * LANES : (j + 1) * LANES].astype(F32)
            total = h * h if total is None else total + h * h
        squares = [jnp.sum(total[k * LANES : (k + 1) * LANES, :].T, axis=0, keepdims=True) for k in range(tiles)]
        acc = jnp.where(srow == 0, jnp.concatenate(squares, axis=1), acc)
        ident = ids[:, part].astype(jnp.int16)
        vals = val[:, part].astype(F32)
        acc = jnp.where(srow == 1, jnp.sum(vals * vals, axis=0, keepdims=True), acc)
        for t in range(STEPS):
            w = [jnp.zeros((K_LOC, LANES), BF16)] * tiles
            for l in range(K_LOC):
                idl = idb[t * K_LOC + l]
                vl = vb[t * K_LOC + l]
                w = [jnp.where(ident[:, k * LANES : (k + 1) * LANES] == idl, vl, w[k]) for k in range(tiles)]
            w = jnp.concatenate(w, axis=1)
            aa = jnp.sum(w.astype(F32) * vals, axis=0, keepdims=True)
            acc = jnp.where(srow == 2 + STEPS + t, aa, acc)
        slot = (d - first) % n
        out[slot, :, 0:step] = acc
        out[slot, :, step:] = tail


def dist_kernel(parts, mind, sums):
    step = mind.shape[1]
    s = parts[0]
    for d in range(1, parts.shape[0]):
        s = s + parts[d]
    sq = s[0:1, 0:step] * s[1:2, 0:step]
    lane = lax.broadcasted_iota(jnp.int32, (1, LANES), 1)
    row = jnp.zeros((1, LANES), F32)
    low = None
    for t in range(STEPS):
        a, b = 2 + t, 2 + STEPS + t
        norm = s[a : a + 1, step : step + 1] * s[b : b + 1, step : step + 1]
        dist = sq + norm - 2.0 * s[a : a + 1, 0:step] * s[b : b + 1, 0:step]
        dist = jnp.maximum(dist, 0.0)
        low = dist if t == 0 else jnp.minimum(low, dist)
        row = jnp.where(lane == t, jnp.sum(low, axis=1, keepdims=True), row)
    mind[...] = low
    sums[...] = jnp.broadcast_to(row, sums.shape)


def pair_kernel(own, other, sums):
    sums[...] = jnp.broadcast_to(own[0:1, :] + other[0:1, :], sums.shape)


def mean_kernel(pool, sums, mind, out, low):
    low[...] = mind[...]
    total = jnp.sum(sums[...], axis=0) / pool
    out[...] = total[0 : out.shape[0]]


def body(hidden_states, factor_values, class_ids, centers):
    rows_all, width = hidden_states.shape
    n_dp, n_mp = lax.axis_size(DP), lax.axis_size(MP)
    n_all = n_dp * n_mp
    rows = rows_all // n_mp
    val = factor_values.T
    ids = class_ids.T
    first = 6
    hbm = pl.BlockSpec(memory_space=pltpu.HBM)

    picked = pl.pallas_call(
        pick_kernel,
        out_shape=jax.ShapeDtypeStruct((n_dp, 32, LANES), BF16),
        in_specs=[hbm] * 4,
        out_specs=vspec(),
        scratch_shapes=[
            pltpu.SMEM((STEPS,), jnp.int32),
            VMEM((STEPS, 8, width), BF16),
            VMEM((STEPS, K_LOC, LANES), BF16),
            VMEM((STEPS, K_LOC, LANES), jnp.int32),
            VMEM((16, LANES), F32),
            pltpu.SemaphoreType.DMA,
            pltpu.SemaphoreType.DMA((STEPS, 3)),
        ],
        compiler_params=params(4),
    )(*(pltpu.with_memory_space_constraint(x, pltpu.HBM) for x in (centers, hidden_states, val, ids)))
    got = lax.all_to_all(picked, DP, 0, 0, tiled=True, axis_index_groups=[led_by(n_dp, 13)])

    parts = pl.pallas_call(
        functools.partial(inner_kernel, first),
        out_shape=jax.ShapeDtypeStruct((n_mp, 8, rows + LANES), F32),
        in_specs=[vspec()] * 4,
        out_specs=vspec(),
        scratch_shapes=[
            VMEM((8, width), F32),
            VMEM((STEPS * K_LOC, K_LOC, LANES), jnp.int16),
            VMEM((STEPS * K_LOC, K_LOC, LANES), BF16),
        ],
        compiler_params=params(24),
    )(got, hidden_states, val, ids)
    parts = lax.all_to_all(parts, MP, 0, 0, tiled=True, axis_index_groups=[led_by(n_mp, first)])

    mind, sums = pl.pallas_call(
        dist_kernel,
        out_shape=[
            VMEM((1, rows), F32),
            jax.ShapeDtypeStruct((1, LANES), F32),
        ],
        in_specs=[vspec()],
        out_specs=[vspec(), vspec()],
        compiler_params=params(4),
    )(parts)
    other = lax.ppermute(sums, "dp_2", [(0, 1), (1, 0)])
    sums = pl.pallas_call(
        pair_kernel,
        out_shape=jax.ShapeDtypeStruct((n_all // 2, LANES), F32),
        in_specs=[vspec(), vspec()],
        out_specs=vspec(),
        compiler_params=params(4),
    )(sums, other)
    sums = lax.all_to_all(sums, ("dp_0", "dp_1", "mp_0", "mp_1"), 0, 0, tiled=True, axis_index_groups=[led_by(n_all // 2, 52)])
    means, mind = pl.pallas_call(
        functools.partial(mean_kernel, rows_all * n_dp),
        out_shape=[jax.ShapeDtypeStruct((STEPS,), F32), jax.ShapeDtypeStruct((1, rows), F32)],
        in_specs=[vspec(), vspec()],
        out_specs=[vspec(), vspec()],
        compiler_params=params(4),
    )(sums, mind)
    return mind.reshape(rows), means


def solution(mesh):
    finer = Mesh(mesh.devices.reshape(2, 4, 2, 4, 2), DP_MP)
    return jax.shard_map(
        body,
        mesh=finer,
        in_specs=(P(DP, MP), P(DP, MP), P(DP, MP), P()),
        out_specs=(P(DP_MP), P()),
        check_vma=False,
    )
```

```python
import functools

import jax
import jax.numpy as jnp
from jax import lax
from jax.experimental import pallas as pl
from jax.experimental.pallas import tpu as pltpu
from jax.sharding import Mesh
from jax.sharding import PartitionSpec as P

K_LOC = 16
STEPS = 3
LANES = 128
MP = ("mp_0", "mp_1")
DP = ("dp_0", "dp_1", "dp_2")
DP_MP = ("dp_0", "dp_1", "dp_2", "mp_0", "mp_1")
VMEM = pltpu.VMEM
F32 = jnp.float32
BF16 = jnp.bfloat16


def led_by(size, first):
    return [(first + i) % size for i in range(size)]


def vspec():
    return pl.BlockSpec(memory_space=VMEM)


def params(mib):
    return pltpu.CompilerParams(vmem_limit_bytes=mib * 1024 * 1024)


def pick_kernel(centers, hid, val, ids, out, cbuf, hbuf, vbuf, ibuf, rows, csem, sem):
    rows_all = hid.shape[0]
    first = pltpu.make_async_copy(centers, cbuf, csem)
    first.start()
    me = lax.axis_index(DP)
    chunks = hid.shape[1] // LANES
    out[...] = jnp.zeros_like(out)
    rows[...] = jnp.zeros_like(rows)
    lane = lax.broadcasted_iota(jnp.int32, (K_LOC, LANES), 1)
    entry = lax.broadcasted_iota(jnp.int32, (K_LOC, LANES), 0)
    first.wait()
    mine = [cbuf[t] // rows_all == me for t in range(STEPS)]

    @pl.when(functools.reduce(jnp.logical_or, mine))
    def _():
        copies = []
        for t in range(STEPS):
            off = lax.rem(cbuf[t], rows_all)
            row8 = pl.multiple_of((off // 8) * 8, 8)
            col = pl.multiple_of((off // LANES) * LANES, LANES)
            copies.append(pltpu.make_async_copy(hid.at[pl.ds(row8, 8), :], hbuf.at[t], sem.at[t, 0]))
            copies.append(pltpu.make_async_copy(val.at[:, pl.ds(col, LANES)], vbuf.at[t], sem.at[t, 1]))
            copies.append(pltpu.make_async_copy(ids.at[:, pl.ds(col, LANES)], ibuf.at[t], sem.at[t, 2]))
        for c in copies:
            c.start()
        for c in copies:
            c.wait()
        for t in range(STEPS):
            off = lax.rem(cbuf[t], rows_all)
            blk = hbuf[t].astype(F32)
            srow = lax.broadcasted_iota(jnp.int32, blk.shape, 0)
            here = srow == jnp.where(mine[t], lax.rem(off, 8), 8)
            row = jnp.sum(jnp.where(here, blk, 0.0), axis=0, keepdims=True)
            for j in range(chunks):
                rows[t * chunks + j : t * chunks + j + 1, :] = row[:, j * LANES : (j + 1) * LANES]
            here = lane == jnp.where(mine[t], lax.rem(off, LANES), LANES)
            vcol = jnp.sum(jnp.where(here, vbuf[t].astype(F32), 0.0), axis=1, keepdims=True)
            icol = jnp.sum(jnp.where(here, ibuf[t], 0), axis=1, keepdims=True)
            parts = (
                vcol,
                (icol >> 16).astype(F32),
                ((icol >> 8) & 255).astype(F32),
                (icol & 255).astype(F32),
            )
            spread = jnp.zeros((K_LOC, LANES), F32)
            for q, part in enumerate(parts):
                spread = jnp.where(lane == K_LOC * q + entry, part, spread)
            at = STEPS * chunks + t
            rows[at : at + 1, :] = jnp.sum(spread, axis=0, keepdims=True)
        tile = rows[...].astype(BF16)
        for d in range(out.shape[0]):
            out[d] = tile


def inner_kernel(first, got, hid, val, ids, out, cvec, idb, vb):
    n = out.shape[0]
    step = hid.shape[0] // n
    chunks = hid.shape[1] // LANES
    lane = lax.broadcasted_iota(jnp.int32, (K_LOC, LANES), 1)
    tile = got[0].astype(F32)
    for d in range(1, got.shape[0]):
        tile = tile + got[d].astype(F32)
    entry = lax.broadcasted_iota(jnp.int32, (K_LOC, LANES), 0)
    cvec[...] = jnp.zeros_like(cvec)
    norms = []
    for t in range(STEPS):
        for j in range(chunks):
            r = t * chunks + j
            cvec[2 + t : 3 + t, j * LANES : (j + 1) * LANES] = tile[r : r + 1, :]
        at = STEPS * chunks + t
        low = jnp.broadcast_to(tile[at : at + 1, :], (K_LOC, LANES))
        cs = [jnp.sum(jnp.where(lane == K_LOC * q + entry, low, 0.0), axis=1, keepdims=True) for q in range(4)]
        idc = (cs[1] * 65536.0 + cs[2] * 256.0 + cs[3]).astype(jnp.int32)
        for l in range(K_LOC):
            idb[t * K_LOC + l] = jnp.broadcast_to(idc[l : l + 1, :], (K_LOC, LANES)).astype(jnp.int16)
            vb[t * K_LOC + l] = jnp.broadcast_to(cs[0][l : l + 1, :], (K_LOC, LANES)).astype(BF16)
        norms.append(jnp.sum(cs[0] * cs[0], axis=0, keepdims=True))
    cmat = cvec[...]
    crow = lax.broadcasted_iota(jnp.int32, (8, LANES), 0)
    tail = jnp.broadcast_to(jnp.sum(cmat * cmat, axis=1, keepdims=True), (8, LANES))
    for t in range(STEPS):
        tail = jnp.where(crow == 2 + STEPS + t, norms[t], tail)
    cb = cmat.astype(BF16)
    srow = lax.broadcasted_iota(jnp.int32, (8, step), 0)
    dims = (((1,), (1,)), ((), ()))
    tiles = step // LANES
    for d in range(n):
        part = slice(d * step, (d + 1) * step)
        acc = lax.dot_general(cb, hid[part, :], dims, preferred_element_type=F32)
        total = None
        for j in range(chunks):
            h = hid[part, j * LANES : (j + 1) * LANES].astype(F32)
            total = h * h if total is None else total + h * h
        squares = [jnp.sum(total[k * LANES : (k + 1) * LANES, :].T, axis=0, keepdims=True) for k in range(tiles)]
        acc = jnp.where(srow == 0, jnp.concatenate(squares, axis=1), acc)
        ident = ids[:, part].astype(jnp.int16)
        vals = val[:, part].astype(F32)
        acc = jnp.where(srow == 1, jnp.sum(vals * vals, axis=0, keepdims=True), acc)
        for t in range(STEPS):
            w = [jnp.zeros((K_LOC, LANES), BF16)] * tiles
            for l in range(K_LOC):
                idl = idb[t * K_LOC + l]
                vl = vb[t * K_LOC + l]
                w = [jnp.where(ident[:, k * LANES : (k + 1) * LANES] == idl, vl, w[k]) for k in range(tiles)]
            w = jnp.concatenate(w, axis=1)
            aa = jnp.sum(w.astype(F32) * vals, axis=0, keepdims=True)
            acc = jnp.where(srow == 2 + STEPS + t, aa, acc)
        slot = (d - first) % n
        out[slot, :, 0:step] = acc
        out[slot, :, step:] = tail


def dist_kernel(parts, mind, sums):
    step = mind.shape[1]
    s = parts[0]
    for d in range(1, parts.shape[0]):
        s = s + parts[d]
    sq = s[0:1, 0:step] * s[1:2, 0:step]
    lane = lax.broadcasted_iota(jnp.int32, (1, LANES), 1)
    row = jnp.zeros((1, LANES), F32)
    low = None
    for t in range(STEPS):
        a, b = 2 + t, 2 + STEPS + t
        norm = s[a : a + 1, step : step + 1] * s[b : b + 1, step : step + 1]
        dist = sq + norm - 2.0 * s[a : a + 1, 0:step] * s[b : b + 1, 0:step]
        dist = jnp.maximum(dist, 0.0)
        low = dist if t == 0 else jnp.minimum(low, dist)
        row = jnp.where(lane == t, jnp.sum(low, axis=1, keepdims=True), row)
    mind[...] = low
    sums[...] = jnp.broadcast_to(row, sums.shape)


def pair_kernel(own, other, sums):
    sums[...] = jnp.broadcast_to(own[0:1, :] + other[0:1, :], sums.shape)


def mean_kernel(pool, sums, mind, out, low):
    low[...] = mind[...]
    total = jnp.sum(sums[...], axis=0) / pool
    out[...] = total[0 : out.shape[0]]


def body(hidden_states, factor_values, class_ids, centers):
    rows_all, width = hidden_states.shape
    n_dp, n_mp = lax.axis_size(DP), lax.axis_size(MP)
    n_all = n_dp * n_mp
    rows = rows_all // n_mp
    val = factor_values.T
    ids = class_ids.T
    first = 6
    hbm = pl.BlockSpec(memory_space=pltpu.HBM)

    picked = pl.pallas_call(
        pick_kernel,
        out_shape=jax.ShapeDtypeStruct((n_dp, 16, LANES), BF16),
        in_specs=[hbm] * 4,
        out_specs=vspec(),
        scratch_shapes=[
            pltpu.SMEM((STEPS,), jnp.int32),
            VMEM((STEPS, 8, width), BF16),
            VMEM((STEPS, K_LOC, LANES), BF16),
            VMEM((STEPS, K_LOC, LANES), jnp.int32),
            VMEM((16, LANES), F32),
            pltpu.SemaphoreType.DMA,
            pltpu.SemaphoreType.DMA((STEPS, 3)),
        ],
        compiler_params=params(4),
    )(*(pltpu.with_memory_space_constraint(x, pltpu.HBM) for x in (centers, hidden_states, val, ids)))
    got = lax.all_to_all(picked, DP, 0, 0, tiled=True, axis_index_groups=[led_by(n_dp, 13)])

    parts = pl.pallas_call(
        functools.partial(inner_kernel, first),
        out_shape=jax.ShapeDtypeStruct((n_mp, 8, rows + LANES), F32),
        in_specs=[vspec()] * 4,
        out_specs=vspec(),
        scratch_shapes=[
            VMEM((8, width), F32),
            VMEM((STEPS * K_LOC, K_LOC, LANES), jnp.int16),
            VMEM((STEPS * K_LOC, K_LOC, LANES), BF16),
        ],
        compiler_params=params(24),
    )(got, hidden_states, val, ids)
    parts = lax.all_to_all(parts, MP, 0, 0, tiled=True, axis_index_groups=[led_by(n_mp, first)])

    mind, sums = pl.pallas_call(
        dist_kernel,
        out_shape=[
            VMEM((1, rows), F32),
            jax.ShapeDtypeStruct((1, LANES), F32),
        ],
        in_specs=[vspec()],
        out_specs=[vspec(), vspec()],
        compiler_params=params(4),
    )(parts)
    other = lax.ppermute(sums, "dp_2", [(0, 1), (1, 0)])
    sums = pl.pallas_call(
        pair_kernel,
        out_shape=jax.ShapeDtypeStruct((n_all // 2, LANES), F32),
        in_specs=[vspec(), vspec()],
        out_specs=vspec(),
        compiler_params=params(4),
    )(sums, other)
    sums = lax.all_to_all(sums, ("dp_0", "dp_1", "mp_0", "mp_1"), 0, 0, tiled=True, axis_index_groups=[led_by(n_all // 2, 52)])
    means, mind = pl.pallas_call(
        functools.partial(mean_kernel, rows_all * n_dp),
        out_shape=[jax.ShapeDtypeStruct((STEPS,), F32), jax.ShapeDtypeStruct((1, rows), F32)],
        in_specs=[vspec(), vspec()],
        out_specs=[vspec(), vspec()],
        compiler_params=params(4),
    )(sums, mind)
    return mind.reshape(rows), means


def solution(mesh):
    finer = Mesh(mesh.devices.reshape(2, 4, 2, 4, 2), DP_MP)
    return jax.shard_map(
        body,
        mesh=finer,
        in_specs=(P(DP, MP), P(DP, MP), P(DP, MP), P()),
        out_specs=(P(DP_MP), P()),
        check_vma=False,
    )
```

```python
import functools

import jax
import jax.numpy as jnp
from jax import lax
from jax.experimental import pallas as pl
from jax.experimental.pallas import tpu as pltpu
from jax.sharding import Mesh
from jax.sharding import PartitionSpec as P

K_LOC = 16
STEPS = 3
LANES = 128
MP = ("mp_0", "mp_1")
DP = ("dp_0", "dp_1", "dp_2")
DP_MP = ("dp_0", "dp_1", "dp_2", "mp_0", "mp_1")
VMEM = pltpu.VMEM
F32 = jnp.float32
BF16 = jnp.bfloat16


def led_by(size, first):
    return [(first + i) % size for i in range(size)]


def vspec():
    return pl.BlockSpec(memory_space=VMEM)


def params(mib):
    return pltpu.CompilerParams(vmem_limit_bytes=mib * 1024 * 1024)


def pick_kernel(centers, hid, val, ids, out, cbuf, hbuf, vbuf, ibuf, rows, csem, sem):
    rows_all = hid.shape[0]
    first = pltpu.make_async_copy(centers, cbuf, csem)
    first.start()
    me = lax.axis_index(DP)
    chunks = hid.shape[1] // LANES
    out[...] = jnp.zeros_like(out)
    rows[...] = jnp.zeros_like(rows)
    lane = lax.broadcasted_iota(jnp.int32, (K_LOC, LANES), 1)
    entry = lax.broadcasted_iota(jnp.int32, (K_LOC, LANES), 0)
    first.wait()
    mine = [cbuf[t] // rows_all == me for t in range(STEPS)]

    def copies(t):
        off = lax.rem(cbuf[t], rows_all)
        row8 = pl.multiple_of((off // 8) * 8, 8)
        col = pl.multiple_of((off // LANES) * LANES, LANES)
        return (
            pltpu.make_async_copy(hid.at[pl.ds(row8, 8), :], hbuf.at[t], sem.at[t, 0]),
            pltpu.make_async_copy(val.at[:, pl.ds(col, LANES)], vbuf.at[t], sem.at[t, 1]),
            pltpu.make_async_copy(ids.at[:, pl.ds(col, LANES)], ibuf.at[t], sem.at[t, 2]),
        )

    for t in range(STEPS):

        @pl.when(mine[t])
        def _(t=t):
            for c in copies(t):
                c.start()

    for t in range(STEPS):

        @pl.when(mine[t])
        def _(t=t):
            for c in copies(t):
                c.wait()
            off = lax.rem(cbuf[t], rows_all)
            blk = hbuf[t].astype(F32)
            here = lax.broadcasted_iota(jnp.int32, blk.shape, 0) == lax.rem(off, 8)
            row = jnp.sum(jnp.where(here, blk, 0.0), axis=0, keepdims=True)
            for j in range(chunks):
                rows[t * chunks + j : t * chunks + j + 1, :] = row[:, j * LANES : (j + 1) * LANES]
            here = lane == lax.rem(off, LANES)
            vcol = jnp.sum(jnp.where(here, vbuf[t].astype(F32), 0.0), axis=1, keepdims=True)
            icol = jnp.sum(jnp.where(here, ibuf[t], 0), axis=1, keepdims=True)
            parts = (
                vcol,
                (icol >> 16).astype(F32),
                ((icol >> 8) & 255).astype(F32),
                (icol & 255).astype(F32),
            )
            spread = jnp.zeros((K_LOC, LANES), F32)
            for q, part in enumerate(parts):
                spread = jnp.where(lane == K_LOC * q + entry, part, spread)
            at = STEPS * chunks + t
            rows[at : at + 1, :] = jnp.sum(spread, axis=0, keepdims=True)

    @pl.when(functools.reduce(jnp.logical_or, mine))
    def _():
        tile = rows[...].astype(BF16)
        for d in range(out.shape[0]):
            out[d] = tile


def inner_kernel(first, got, hid, val, ids, out, cvec, idb, vb):
    n = out.shape[0]
    step = hid.shape[0] // n
    chunks = hid.shape[1] // LANES
    lane = lax.broadcasted_iota(jnp.int32, (K_LOC, LANES), 1)
    tile = got[0].astype(F32)
    for d in range(1, got.shape[0]):
        tile = tile + got[d].astype(F32)
    entry = lax.broadcasted_iota(jnp.int32, (K_LOC, LANES), 0)
    cvec[...] = jnp.zeros_like(cvec)
    norms = []
    for t in range(STEPS):
        for j in range(chunks):
            r = t * chunks + j
            cvec[2 + t : 3 + t, j * LANES : (j + 1) * LANES] = tile[r : r + 1, :]
        at = STEPS * chunks + t
        low = jnp.broadcast_to(tile[at : at + 1, :], (K_LOC, LANES))
        cs = [jnp.sum(jnp.where(lane == K_LOC * q + entry, low, 0.0), axis=1, keepdims=True) for q in range(4)]
        idc = (cs[1] * 65536.0 + cs[2] * 256.0 + cs[3]).astype(jnp.int32)
        for l in range(K_LOC):
            idb[t * K_LOC + l] = jnp.broadcast_to(idc[l : l + 1, :], (K_LOC, LANES)).astype(jnp.int16)
            vb[t * K_LOC + l] = jnp.broadcast_to(cs[0][l : l + 1, :], (K_LOC, LANES)).astype(BF16)
        norms.append(jnp.sum(cs[0] * cs[0], axis=0, keepdims=True))
    cmat = cvec[...]
    crow = lax.broadcasted_iota(jnp.int32, (8, LANES), 0)
    tail = jnp.broadcast_to(jnp.sum(cmat * cmat, axis=1, keepdims=True), (8, LANES))
    for t in range(STEPS):
        tail = jnp.where(crow == 2 + STEPS + t, norms[t], tail)
    cb = cmat.astype(BF16)
    srow = lax.broadcasted_iota(jnp.int32, (8, step), 0)
    dims = (((1,), (1,)), ((), ()))
    tiles = step // LANES
    for d in range(n):
        part = slice(d * step, (d + 1) * step)
        acc = lax.dot_general(cb, hid[part, :], dims, preferred_element_type=F32)
        total = None
        for j in range(chunks):
            h = hid[part, j * LANES : (j + 1) * LANES].astype(F32)
            total = h * h if total is None else total + h * h
        squares = [jnp.sum(total[k * LANES : (k + 1) * LANES, :].T, axis=0, keepdims=True) for k in range(tiles)]
        acc = jnp.where(srow == 0, jnp.concatenate(squares, axis=1), acc)
        ident = ids[:, part].astype(jnp.int16)
        vals = val[:, part].astype(F32)
        acc = jnp.where(srow == 1, jnp.sum(vals * vals, axis=0, keepdims=True), acc)
        for t in range(STEPS):
            w = [jnp.zeros((K_LOC, LANES), BF16)] * tiles
            for l in range(K_LOC):
                idl = idb[t * K_LOC + l]
                vl = vb[t * K_LOC + l]
                w = [jnp.where(ident[:, k * LANES : (k + 1) * LANES] == idl, vl, w[k]) for k in range(tiles)]
            w = jnp.concatenate(w, axis=1)
            aa = jnp.sum(w.astype(F32) * vals, axis=0, keepdims=True)
            acc = jnp.where(srow == 2 + STEPS + t, aa, acc)
        slot = (d - first) % n
        out[slot, :, 0:step] = acc
        out[slot, :, step:] = tail


def dist_kernel(parts, mind, sums):
    step = mind.shape[1]
    s = parts[0]
    for d in range(1, parts.shape[0]):
        s = s + parts[d]
    sq = s[0:1, 0:step] * s[1:2, 0:step]
    lane = lax.broadcasted_iota(jnp.int32, (1, LANES), 1)
    row = jnp.zeros((1, LANES), F32)
    low = None
    for t in range(STEPS):
        a, b = 2 + t, 2 + STEPS + t
        norm = s[a : a + 1, step : step + 1] * s[b : b + 1, step : step + 1]
        dist = sq + norm - 2.0 * s[a : a + 1, 0:step] * s[b : b + 1, 0:step]
        dist = jnp.maximum(dist, 0.0)
        low = dist if t == 0 else jnp.minimum(low, dist)
        row = jnp.where(lane == t, jnp.sum(low, axis=1, keepdims=True), row)
    mind[...] = low
    sums[...] = jnp.broadcast_to(row, sums.shape)


def pair_kernel(own, other, sums):
    sums[...] = jnp.broadcast_to(own[0:1, :] + other[0:1, :], sums.shape)


def mean_kernel(pool, sums, mind, out, low):
    low[...] = mind[...]
    total = jnp.sum(sums[...], axis=0) / pool
    out[...] = total[0 : out.shape[0]]


def body(hidden_states, factor_values, class_ids, centers):
    rows_all, width = hidden_states.shape
    n_dp, n_mp = lax.axis_size(DP), lax.axis_size(MP)
    n_all = n_dp * n_mp
    rows = rows_all // n_mp
    val = factor_values.T
    ids = class_ids.T
    first = 6
    hbm = pl.BlockSpec(memory_space=pltpu.HBM)

    picked = pl.pallas_call(
        pick_kernel,
        out_shape=jax.ShapeDtypeStruct((n_dp, 16, LANES), BF16),
        in_specs=[hbm] * 4,
        out_specs=vspec(),
        scratch_shapes=[
            pltpu.SMEM((STEPS,), jnp.int32),
            VMEM((STEPS, 8, width), BF16),
            VMEM((STEPS, K_LOC, LANES), BF16),
            VMEM((STEPS, K_LOC, LANES), jnp.int32),
            VMEM((16, LANES), F32),
            pltpu.SemaphoreType.DMA,
            pltpu.SemaphoreType.DMA((STEPS, 3)),
        ],
        compiler_params=params(4),
    )(*(pltpu.with_memory_space_constraint(x, pltpu.HBM) for x in (centers, hidden_states, val, ids)))
    got = lax.all_to_all(picked, DP, 0, 0, tiled=True, axis_index_groups=[led_by(n_dp, 13)])

    parts = pl.pallas_call(
        functools.partial(inner_kernel, first),
        out_shape=jax.ShapeDtypeStruct((n_mp, 8, rows + LANES), F32),
        in_specs=[vspec()] * 4,
        out_specs=vspec(),
        scratch_shapes=[
            VMEM((8, width), F32),
            VMEM((STEPS * K_LOC, K_LOC, LANES), jnp.int16),
            VMEM((STEPS * K_LOC, K_LOC, LANES), BF16),
        ],
        compiler_params=params(24),
    )(got, hidden_states, val, ids)
    parts = lax.all_to_all(parts, MP, 0, 0, tiled=True, axis_index_groups=[led_by(n_mp, first)])

    mind, sums = pl.pallas_call(
        dist_kernel,
        out_shape=[
            VMEM((1, rows), F32),
            jax.ShapeDtypeStruct((1, LANES), F32),
        ],
        in_specs=[vspec()],
        out_specs=[vspec(), vspec()],
        compiler_params=params(4),
    )(parts)
    other = lax.ppermute(sums, "dp_2", [(0, 1), (1, 0)])
    sums = pl.pallas_call(
        pair_kernel,
        out_shape=jax.ShapeDtypeStruct((n_all // 2, LANES), F32),
        in_specs=[vspec(), vspec()],
        out_specs=vspec(),
        compiler_params=params(4),
    )(sums, other)
    sums = lax.all_to_all(sums, ("dp_0", "dp_1", "mp_0", "mp_1"), 0, 0, tiled=True, axis_index_groups=[led_by(n_all // 2, 52)])
    means, mind = pl.pallas_call(
        functools.partial(mean_kernel, rows_all * n_dp),
        out_shape=[jax.ShapeDtypeStruct((STEPS,), F32), jax.ShapeDtypeStruct((1, rows), F32)],
        in_specs=[vspec(), vspec()],
        out_specs=[vspec(), vspec()],
        compiler_params=params(4),
    )(sums, mind)
    return mind.reshape(rows), means


def solution(mesh):
    finer = Mesh(mesh.devices.reshape(2, 4, 2, 4, 2), DP_MP)
    return jax.shard_map(
        body,
        mesh=finer,
        in_specs=(P(DP, MP), P(DP, MP), P(DP, MP), P()),
        out_specs=(P(DP_MP), P()),
        check_vma=False,
    )
```

```python
import functools

import jax
import jax.numpy as jnp
from jax import lax
from jax.experimental import pallas as pl
from jax.experimental.pallas import tpu as pltpu
from jax.sharding import Mesh
from jax.sharding import PartitionSpec as P

K_LOC = 16
STEPS = 3
LANES = 128
MP = ("mp_0", "mp_1")
DP = ("dp_0", "dp_1", "dp_2")
DP_MP = ("dp_0", "dp_1", "dp_2", "mp_0", "mp_1")
VMEM = pltpu.VMEM
F32 = jnp.float32
BF16 = jnp.bfloat16


def led_by(size, first):
    return [(first + i) % size for i in range(size)]


def vspec():
    return pl.BlockSpec(memory_space=VMEM)


def params(mib):
    return pltpu.CompilerParams(vmem_limit_bytes=mib * 1024 * 1024)


def pick_kernel(centers, hid, val, ids, out, cbuf, hbuf, vbuf, ibuf, rows, csem, sem):
    rows_all = hid.shape[0]
    first = pltpu.make_async_copy(centers, cbuf, csem)
    first.start()
    me = lax.axis_index(DP)
    chunks = hid.shape[1] // LANES
    out[...] = jnp.zeros_like(out)
    rows[...] = jnp.zeros_like(rows)
    lane = lax.broadcasted_iota(jnp.int32, (K_LOC, LANES), 1)
    entry = lax.broadcasted_iota(jnp.int32, (K_LOC, LANES), 0)
    first.wait()
    mine = [cbuf[t] // rows_all == me for t in range(STEPS)]

    def copies(t):
        off = lax.rem(cbuf[t], rows_all)
        row8 = pl.multiple_of((off // 8) * 8, 8)
        col = pl.multiple_of((off // LANES) * LANES, LANES)
        return (
            pltpu.make_async_copy(hid.at[pl.ds(row8, 8), :], hbuf.at[t], sem.at[t, 0]),
            pltpu.make_async_copy(val.at[:, pl.ds(col, LANES)], vbuf.at[t], sem.at[t, 1]),
            pltpu.make_async_copy(ids.at[:, pl.ds(col, LANES)], ibuf.at[t], sem.at[t, 2]),
        )

    @pl.when(functools.reduce(jnp.logical_or, mine))
    def _():
        for t in range(STEPS):

            @pl.when(mine[t])
            def _(t=t):
                for c in copies(t):
                    c.start()

        for t in range(STEPS):

            @pl.when(mine[t])
            def _(t=t):
                for c in copies(t):
                    c.wait()
                off = lax.rem(cbuf[t], rows_all)
                blk = hbuf[t].astype(F32)
                here = lax.broadcasted_iota(jnp.int32, blk.shape, 0) == lax.rem(off, 8)
                row = jnp.sum(jnp.where(here, blk, 0.0), axis=0, keepdims=True)
                for j in range(chunks):
                    rows[t * chunks + j : t * chunks + j + 1, :] = row[:, j * LANES : (j + 1) * LANES]
                here = lane == lax.rem(off, LANES)
                vcol = jnp.sum(jnp.where(here, vbuf[t].astype(F32), 0.0), axis=1, keepdims=True)
                icol = jnp.sum(jnp.where(here, ibuf[t], 0), axis=1, keepdims=True)
                parts = (
                    vcol,
                    (icol >> 16).astype(F32),
                    ((icol >> 8) & 255).astype(F32),
                    (icol & 255).astype(F32),
                )
                spread = jnp.zeros((K_LOC, LANES), F32)
                for q, part in enumerate(parts):
                    spread = jnp.where(lane == K_LOC * q + entry, part, spread)
                at = STEPS * chunks + t
                rows[at : at + 1, :] = jnp.sum(spread, axis=0, keepdims=True)

        tile = rows[...].astype(BF16)
        for d in range(out.shape[0]):
            out[d] = tile


def inner_kernel(first, got, hid, val, ids, out, cvec, idb, vb):
    n = out.shape[0]
    step = hid.shape[0] // n
    chunks = hid.shape[1] // LANES
    lane = lax.broadcasted_iota(jnp.int32, (K_LOC, LANES), 1)
    tile = got[0].astype(F32)
    for d in range(1, got.shape[0]):
        tile = tile + got[d].astype(F32)
    entry = lax.broadcasted_iota(jnp.int32, (K_LOC, LANES), 0)
    cvec[...] = jnp.zeros_like(cvec)
    norms = []
    for t in range(STEPS):
        for j in range(chunks):
            r = t * chunks + j
            cvec[2 + t : 3 + t, j * LANES : (j + 1) * LANES] = tile[r : r + 1, :]
        at = STEPS * chunks + t
        low = jnp.broadcast_to(tile[at : at + 1, :], (K_LOC, LANES))
        cs = [jnp.sum(jnp.where(lane == K_LOC * q + entry, low, 0.0), axis=1, keepdims=True) for q in range(4)]
        idc = (cs[1] * 65536.0 + cs[2] * 256.0 + cs[3]).astype(jnp.int32)
        for l in range(K_LOC):
            idb[t * K_LOC + l] = jnp.broadcast_to(idc[l : l + 1, :], (K_LOC, LANES)).astype(jnp.int16)
            vb[t * K_LOC + l] = jnp.broadcast_to(cs[0][l : l + 1, :], (K_LOC, LANES)).astype(BF16)
        norms.append(jnp.sum(cs[0] * cs[0], axis=0, keepdims=True))
    cmat = cvec[...]
    crow = lax.broadcasted_iota(jnp.int32, (8, LANES), 0)
    tail = jnp.broadcast_to(jnp.sum(cmat * cmat, axis=1, keepdims=True), (8, LANES))
    for t in range(STEPS):
        tail = jnp.where(crow == 2 + STEPS + t, norms[t], tail)
    cb = cmat.astype(BF16)
    srow = lax.broadcasted_iota(jnp.int32, (8, step), 0)
    dims = (((1,), (1,)), ((), ()))
    tiles = step // LANES
    for d in range(n):
        part = slice(d * step, (d + 1) * step)
        acc = lax.dot_general(cb, hid[part, :], dims, preferred_element_type=F32)
        total = None
        for j in range(chunks):
            h = hid[part, j * LANES : (j + 1) * LANES].astype(F32)
            total = h * h if total is None else total + h * h
        squares = [jnp.sum(total[k * LANES : (k + 1) * LANES, :].T, axis=0, keepdims=True) for k in range(tiles)]
        acc = jnp.where(srow == 0, jnp.concatenate(squares, axis=1), acc)
        ident = ids[:, part].astype(jnp.int16)
        vals = val[:, part].astype(F32)
        acc = jnp.where(srow == 1, jnp.sum(vals * vals, axis=0, keepdims=True), acc)
        for t in range(STEPS):
            w = [jnp.zeros((K_LOC, LANES), BF16)] * tiles
            for l in range(K_LOC):
                idl = idb[t * K_LOC + l]
                vl = vb[t * K_LOC + l]
                w = [jnp.where(ident[:, k * LANES : (k + 1) * LANES] == idl, vl, w[k]) for k in range(tiles)]
            w = jnp.concatenate(w, axis=1)
            aa = jnp.sum(w.astype(F32) * vals, axis=0, keepdims=True)
            acc = jnp.where(srow == 2 + STEPS + t, aa, acc)
        slot = (d - first) % n
        out[slot, :, 0:step] = acc
        out[slot, :, step:] = tail


def dist_kernel(parts, mind, sums):
    step = mind.shape[1]
    s = parts[0]
    for d in range(1, parts.shape[0]):
        s = s + parts[d]
    sq = s[0:1, 0:step] * s[1:2, 0:step]
    lane = lax.broadcasted_iota(jnp.int32, (1, LANES), 1)
    row = jnp.zeros((1, LANES), F32)
    low = None
    for t in range(STEPS):
        a, b = 2 + t, 2 + STEPS + t
        norm = s[a : a + 1, step : step + 1] * s[b : b + 1, step : step + 1]
        dist = sq + norm - 2.0 * s[a : a + 1, 0:step] * s[b : b + 1, 0:step]
        dist = jnp.maximum(dist, 0.0)
        low = dist if t == 0 else jnp.minimum(low, dist)
        row = jnp.where(lane == t, jnp.sum(low, axis=1, keepdims=True), row)
    mind[...] = low
    sums[...] = jnp.broadcast_to(row, sums.shape)


def pair_kernel(own, other, sums):
    sums[...] = jnp.broadcast_to(own[0:1, :] + other[0:1, :], sums.shape)


def mean_kernel(pool, sums, mind, out, low):
    low[...] = mind[...]
    total = jnp.sum(sums[...], axis=0) / pool
    out[...] = total[0 : out.shape[0]]


def body(hidden_states, factor_values, class_ids, centers):
    rows_all, width = hidden_states.shape
    n_dp, n_mp = lax.axis_size(DP), lax.axis_size(MP)
    n_all = n_dp * n_mp
    rows = rows_all // n_mp
    val = factor_values.T
    ids = class_ids.T
    first = 6
    hbm = pl.BlockSpec(memory_space=pltpu.HBM)

    picked = pl.pallas_call(
        pick_kernel,
        out_shape=jax.ShapeDtypeStruct((n_dp, 16, LANES), BF16),
        in_specs=[hbm] * 4,
        out_specs=vspec(),
        scratch_shapes=[
            pltpu.SMEM((STEPS,), jnp.int32),
            VMEM((STEPS, 8, width), BF16),
            VMEM((STEPS, K_LOC, LANES), BF16),
            VMEM((STEPS, K_LOC, LANES), jnp.int32),
            VMEM((16, LANES), F32),
            pltpu.SemaphoreType.DMA,
            pltpu.SemaphoreType.DMA((STEPS, 3)),
        ],
        compiler_params=params(4),
    )(*(pltpu.with_memory_space_constraint(x, pltpu.HBM) for x in (centers, hidden_states, val, ids)))
    got = lax.all_to_all(picked, DP, 0, 0, tiled=True, axis_index_groups=[led_by(n_dp, 13)])

    parts = pl.pallas_call(
        functools.partial(inner_kernel, first),
        out_shape=jax.ShapeDtypeStruct((n_mp, 8, rows + LANES), F32),
        in_specs=[vspec()] * 4,
        out_specs=vspec(),
        scratch_shapes=[
            VMEM((8, width), F32),
            VMEM((STEPS * K_LOC, K_LOC, LANES), jnp.int16),
            VMEM((STEPS * K_LOC, K_LOC, LANES), BF16),
        ],
        compiler_params=params(24),
    )(got, hidden_states, val, ids)
    parts = lax.all_to_all(parts, MP, 0, 0, tiled=True, axis_index_groups=[led_by(n_mp, first)])

    mind, sums = pl.pallas_call(
        dist_kernel,
        out_shape=[
            VMEM((1, rows), F32),
            jax.ShapeDtypeStruct((1, LANES), F32),
        ],
        in_specs=[vspec()],
        out_specs=[vspec(), vspec()],
        compiler_params=params(4),
    )(parts)
    other = lax.ppermute(sums, "dp_2", [(0, 1), (1, 0)])
    sums = pl.pallas_call(
        pair_kernel,
        out_shape=jax.ShapeDtypeStruct((n_all // 2, LANES), F32),
        in_specs=[vspec(), vspec()],
        out_specs=vspec(),
        compiler_params=params(4),
    )(sums, other)
    sums = lax.all_to_all(sums, ("dp_0", "dp_1", "mp_0", "mp_1"), 0, 0, tiled=True, axis_index_groups=[led_by(n_all // 2, 52)])
    means, mind = pl.pallas_call(
        functools.partial(mean_kernel, rows_all * n_dp),
        out_shape=[jax.ShapeDtypeStruct((STEPS,), F32), jax.ShapeDtypeStruct((1, rows), F32)],
        in_specs=[vspec(), vspec()],
        out_specs=[vspec(), vspec()],
        compiler_params=params(4),
    )(sums, mind)
    return mind.reshape(rows), means


def solution(mesh):
    finer = Mesh(mesh.devices.reshape(2, 4, 2, 4, 2), DP_MP)
    return jax.shard_map(
        body,
        mesh=finer,
        in_specs=(P(DP, MP), P(DP, MP), P(DP, MP), P()),
        out_specs=(P(DP_MP), P()),
        check_vma=False,
    )
```

```python
import functools

import jax
import jax.numpy as jnp
from jax import lax
from jax.experimental import pallas as pl
from jax.experimental.pallas import tpu as pltpu
from jax.sharding import Mesh
from jax.sharding import PartitionSpec as P

K_LOC = 16
STEPS = 3
LANES = 128
MP = ("mp_0", "mp_1")
DP = ("dp_0", "dp_1", "dp_2")
DP_MP = ("dp_0", "dp_1", "dp_2", "mp_0", "mp_1")
VMEM = pltpu.VMEM
F32 = jnp.float32
BF16 = jnp.bfloat16


def led_by(size, first):
    return [(first + i) % size for i in range(size)]


def vspec():
    return pl.BlockSpec(memory_space=VMEM)


def params(mib):
    return pltpu.CompilerParams(vmem_limit_bytes=mib * 1024 * 1024)


def pick_kernel(centers, hid, val, ids, out, cbuf, hbuf, vbuf, ibuf, rows, csem, sem):
    rows_all = hid.shape[0]
    first = pltpu.make_async_copy(centers, cbuf, csem)
    first.start()
    me = lax.axis_index(DP)
    chunks = hid.shape[1] // LANES
    out[...] = jnp.zeros_like(out)
    rows[...] = jnp.zeros_like(rows)
    lane = lax.broadcasted_iota(jnp.int32, (K_LOC, LANES), 1)
    entry = lax.broadcasted_iota(jnp.int32, (K_LOC, LANES), 0)
    first.wait()
    mine = [cbuf[t] // rows_all == me for t in range(STEPS)]

    def copies(t):
        off = lax.rem(cbuf[t], rows_all)
        row8 = pl.multiple_of((off // 8) * 8, 8)
        col = pl.multiple_of((off // LANES) * LANES, LANES)
        return (
            pltpu.make_async_copy(hid.at[pl.ds(row8, 8), :], hbuf.at[t], sem.at[t, 0]),
            pltpu.make_async_copy(val.at[:, pl.ds(col, LANES)], vbuf.at[t], sem.at[t, 1]),
            pltpu.make_async_copy(ids.at[:, pl.ds(col, LANES)], ibuf.at[t], sem.at[t, 2]),
        )

    @pl.when(functools.reduce(jnp.logical_or, mine))
    def _():
        for t in range(STEPS):

            @pl.when(mine[t])
            def _(t=t):
                for c in copies(t):
                    c.start()

        for t in range(STEPS):

            @pl.when(mine[t])
            def _(t=t):
                for c in copies(t):
                    c.wait()
                off = lax.rem(cbuf[t], rows_all)
                blk = hbuf[t].astype(F32)
                here = lax.broadcasted_iota(jnp.int32, blk.shape, 0) == lax.rem(off, 8)
                row = jnp.sum(jnp.where(here, blk, 0.0), axis=0, keepdims=True)
                for j in range(chunks):
                    rows[t * chunks + j : t * chunks + j + 1, :] = row[:, j * LANES : (j + 1) * LANES]
                here = lane == lax.rem(off, LANES)
                vcol = jnp.sum(jnp.where(here, vbuf[t].astype(F32), 0.0), axis=1, keepdims=True)
                icol = jnp.sum(jnp.where(here, ibuf[t], 0), axis=1, keepdims=True)
                parts = (
                    vcol,
                    (icol >> 16).astype(F32),
                    ((icol >> 8) & 255).astype(F32),
                    (icol & 255).astype(F32),
                )
                spread = jnp.zeros((K_LOC, LANES), F32)
                for q, part in enumerate(parts):
                    spread = jnp.where(lane == K_LOC * q + entry, part, spread)
                at = STEPS * chunks + t
                rows[at : at + 1, :] = jnp.sum(spread, axis=0, keepdims=True)

        tile = rows[...].astype(BF16)
        for d in range(out.shape[0]):
            out[d] = tile


def inner_kernel(order, got, hid, val, ids, out, cvec, idb, vb):
    n = out.shape[0]
    step = hid.shape[0] // n
    chunks = hid.shape[1] // LANES
    lane = lax.broadcasted_iota(jnp.int32, (K_LOC, LANES), 1)
    tile = got[0].astype(F32)
    for d in range(1, got.shape[0]):
        tile = tile + got[d].astype(F32)
    entry = lax.broadcasted_iota(jnp.int32, (K_LOC, LANES), 0)
    cvec[...] = jnp.zeros_like(cvec)
    norms = []
    for t in range(STEPS):
        for j in range(chunks):
            r = t * chunks + j
            cvec[2 + t : 3 + t, j * LANES : (j + 1) * LANES] = tile[r : r + 1, :]
        at = STEPS * chunks + t
        low = jnp.broadcast_to(tile[at : at + 1, :], (K_LOC, LANES))
        cs = [jnp.sum(jnp.where(lane == K_LOC * q + entry, low, 0.0), axis=1, keepdims=True) for q in range(4)]
        idc = (cs[1] * 65536.0 + cs[2] * 256.0 + cs[3]).astype(jnp.int32)
        for l in range(K_LOC):
            idb[t * K_LOC + l] = jnp.broadcast_to(idc[l : l + 1, :], (K_LOC, LANES)).astype(jnp.int16)
            vb[t * K_LOC + l] = jnp.broadcast_to(cs[0][l : l + 1, :], (K_LOC, LANES)).astype(BF16)
        norms.append(jnp.sum(cs[0] * cs[0], axis=0, keepdims=True))
    cmat = cvec[...]
    crow = lax.broadcasted_iota(jnp.int32, (8, LANES), 0)
    tail = jnp.broadcast_to(jnp.sum(cmat * cmat, axis=1, keepdims=True), (8, LANES))
    for t in range(STEPS):
        tail = jnp.where(crow == 2 + STEPS + t, norms[t], tail)
    cb = cmat.astype(BF16)
    srow = lax.broadcasted_iota(jnp.int32, (8, step), 0)
    dims = (((1,), (1,)), ((), ()))
    tiles = step // LANES
    for d in range(n):
        part = slice(d * step, (d + 1) * step)
        acc = lax.dot_general(cb, hid[part, :], dims, preferred_element_type=F32)
        total = None
        for j in range(chunks):
            h = hid[part, j * LANES : (j + 1) * LANES].astype(F32)
            total = h * h if total is None else total + h * h
        squares = [jnp.sum(total[k * LANES : (k + 1) * LANES, :].T, axis=0, keepdims=True) for k in range(tiles)]
        acc = jnp.where(srow == 0, jnp.concatenate(squares, axis=1), acc)
        ident = ids[:, part].astype(jnp.int16)
        vals = val[:, part].astype(F32)
        acc = jnp.where(srow == 1, jnp.sum(vals * vals, axis=0, keepdims=True), acc)
        for t in range(STEPS):
            w = [jnp.zeros((K_LOC, LANES), BF16)] * tiles
            for l in range(K_LOC):
                idl = idb[t * K_LOC + l]
                vl = vb[t * K_LOC + l]
                w = [jnp.where(ident[:, k * LANES : (k + 1) * LANES] == idl, vl, w[k]) for k in range(tiles)]
            w = jnp.concatenate(w, axis=1)
            aa = jnp.sum(w.astype(F32) * vals, axis=0, keepdims=True)
            acc = jnp.where(srow == 2 + STEPS + t, aa, acc)
        slot = order.index(d)
        out[slot, :, 0:step] = acc
        out[slot, :, step:] = tail


def dist_kernel(parts, mind, sums):
    step = mind.shape[1]
    s = parts[0]
    for d in range(1, parts.shape[0]):
        s = s + parts[d]
    sq = s[0:1, 0:step] * s[1:2, 0:step]
    lane = lax.broadcasted_iota(jnp.int32, (1, LANES), 1)
    row = jnp.zeros((1, LANES), F32)
    low = None
    for t in range(STEPS):
        a, b = 2 + t, 2 + STEPS + t
        norm = s[a : a + 1, step : step + 1] * s[b : b + 1, step : step + 1]
        dist = sq + norm - 2.0 * s[a : a + 1, 0:step] * s[b : b + 1, 0:step]
        dist = jnp.maximum(dist, 0.0)
        low = dist if t == 0 else jnp.minimum(low, dist)
        row = jnp.where(lane == t, jnp.sum(low, axis=1, keepdims=True), row)
    mind[...] = low
    sums[...] = jnp.broadcast_to(row, sums.shape)


def pair_kernel(own, other, sums):
    sums[...] = jnp.broadcast_to(own[0:1, :] + other[0:1, :], sums.shape)


def mean_kernel(pool, sums, mind, out, low):
    low[...] = mind[...]
    total = jnp.sum(sums[...], axis=0) / pool
    out[...] = total[0 : out.shape[0]]


def body(hidden_states, factor_values, class_ids, centers):
    rows_all, width = hidden_states.shape
    n_dp, n_mp = lax.axis_size(DP), lax.axis_size(MP)
    n_all = n_dp * n_mp
    rows = rows_all // n_mp
    val = factor_values.T
    ids = class_ids.T
    order = [6, 4, 0, 2, 7, 5, 1, 3]
    hbm = pl.BlockSpec(memory_space=pltpu.HBM)

    picked = pl.pallas_call(
        pick_kernel,
        out_shape=jax.ShapeDtypeStruct((n_dp, 16, LANES), BF16),
        in_specs=[hbm] * 4,
        out_specs=vspec(),
        scratch_shapes=[
            pltpu.SMEM((STEPS,), jnp.int32),
            VMEM((STEPS, 8, width), BF16),
            VMEM((STEPS, K_LOC, LANES), BF16),
            VMEM((STEPS, K_LOC, LANES), jnp.int32),
            VMEM((16, LANES), F32),
            pltpu.SemaphoreType.DMA,
            pltpu.SemaphoreType.DMA((STEPS, 3)),
        ],
        compiler_params=params(4),
    )(*(pltpu.with_memory_space_constraint(x, pltpu.HBM) for x in (centers, hidden_states, val, ids)))
    got = lax.all_to_all(picked, DP, 0, 0, tiled=True, axis_index_groups=[led_by(n_dp, 13)])

    parts = pl.pallas_call(
        functools.partial(inner_kernel, order),
        out_shape=jax.ShapeDtypeStruct((n_mp, 8, rows + LANES), F32),
        in_specs=[vspec()] * 4,
        out_specs=vspec(),
        scratch_shapes=[
            VMEM((8, width), F32),
            VMEM((STEPS * K_LOC, K_LOC, LANES), jnp.int16),
            VMEM((STEPS * K_LOC, K_LOC, LANES), BF16),
        ],
        compiler_params=params(24),
    )(got, hidden_states, val, ids)
    parts = lax.all_to_all(parts, MP, 0, 0, tiled=True, axis_index_groups=[order])

    mind, sums = pl.pallas_call(
        dist_kernel,
        out_shape=[
            VMEM((1, rows), F32),
            jax.ShapeDtypeStruct((1, LANES), F32),
        ],
        in_specs=[vspec()],
        out_specs=[vspec(), vspec()],
        compiler_params=params(4),
    )(parts)
    other = lax.ppermute(sums, "dp_2", [(0, 1), (1, 0)])
    sums = pl.pallas_call(
        pair_kernel,
        out_shape=jax.ShapeDtypeStruct((n_all // 2, LANES), F32),
        in_specs=[vspec(), vspec()],
        out_specs=vspec(),
        compiler_params=params(4),
    )(sums, other)
    sums = lax.all_to_all(sums, ("dp_0", "dp_1", "mp_0", "mp_1"), 0, 0, tiled=True, axis_index_groups=[led_by(n_all // 2, 52)])
    means, mind = pl.pallas_call(
        functools.partial(mean_kernel, rows_all * n_dp),
        out_shape=[jax.ShapeDtypeStruct((STEPS,), F32), jax.ShapeDtypeStruct((1, rows), F32)],
        in_specs=[vspec(), vspec()],
        out_specs=[vspec(), vspec()],
        compiler_params=params(4),
    )(sums, mind)
    return mind.reshape(rows), means


def solution(mesh):
    finer = Mesh(mesh.devices.reshape(2, 4, 2, 4, 2), DP_MP)
    return jax.shard_map(
        body,
        mesh=finer,
        in_specs=(P(DP, MP), P(DP, MP), P(DP, MP), P()),
        out_specs=(P(DP_MP), P()),
        check_vma=False,
    )
```

```python
import functools

import jax
import jax.numpy as jnp
from jax import lax
from jax.experimental import pallas as pl
from jax.experimental.pallas import tpu as pltpu
from jax.sharding import Mesh
from jax.sharding import PartitionSpec as P

K_LOC = 16
STEPS = 3
LANES = 128
MP = ("mp_0", "mp_1")
DP = ("dp_0", "dp_1", "dp_2")
DP_MP = ("dp_0", "dp_1", "dp_2", "mp_0", "mp_1")
VMEM = pltpu.VMEM
F32 = jnp.float32
BF16 = jnp.bfloat16


def led_by(size, first):
    return [(first + i) % size for i in range(size)]


def vspec():
    return pl.BlockSpec(memory_space=VMEM)


def params(mib):
    return pltpu.CompilerParams(vmem_limit_bytes=mib * 1024 * 1024)


def pick_kernel(centers, hid, val, ids, out, cbuf, hbuf, vbuf, ibuf, rows, csem, sem):
    rows_all = hid.shape[0]
    first = pltpu.make_async_copy(centers, cbuf, csem)
    first.start()
    me = lax.axis_index(DP)
    chunks = hid.shape[1] // LANES
    out[...] = jnp.zeros_like(out)
    rows[...] = jnp.zeros_like(rows)
    lane = lax.broadcasted_iota(jnp.int32, (K_LOC, LANES), 1)
    entry = lax.broadcasted_iota(jnp.int32, (K_LOC, LANES), 0)
    first.wait()
    mine = [cbuf[t] // rows_all == me for t in range(STEPS)]

    def copies(t):
        off = lax.rem(cbuf[t], rows_all)
        row8 = pl.multiple_of((off // 8) * 8, 8)
        col = pl.multiple_of((off // LANES) * LANES, LANES)
        return (
            pltpu.make_async_copy(hid.at[pl.ds(row8, 8), :], hbuf.at[t], sem.at[t, 0]),
            pltpu.make_async_copy(val.at[:, pl.ds(col, LANES)], vbuf.at[t], sem.at[t, 1]),
            pltpu.make_async_copy(ids.at[:, pl.ds(col, LANES)], ibuf.at[t], sem.at[t, 2]),
        )

    @pl.when(functools.reduce(jnp.logical_or, mine))
    def _():
        for t in range(STEPS):

            @pl.when(mine[t])
            def _(t=t):
                for c in copies(t):
                    c.start()

        for t in range(STEPS):

            @pl.when(mine[t])
            def _(t=t):
                for c in copies(t):
                    c.wait()
                off = lax.rem(cbuf[t], rows_all)
                blk = hbuf[t].astype(F32)
                here = lax.broadcasted_iota(jnp.int32, blk.shape, 0) == lax.rem(off, 8)
                row = jnp.sum(jnp.where(here, blk, 0.0), axis=0, keepdims=True)
                for j in range(chunks):
                    rows[t * chunks + j : t * chunks + j + 1, :] = row[:, j * LANES : (j + 1) * LANES]
                here = lane == lax.rem(off, LANES)
                vcol = jnp.sum(jnp.where(here, vbuf[t].astype(F32), 0.0), axis=1, keepdims=True)
                icol = jnp.sum(jnp.where(here, ibuf[t], 0), axis=1, keepdims=True)
                parts = (
                    vcol,
                    (icol >> 16).astype(F32),
                    ((icol >> 8) & 255).astype(F32),
                    (icol & 255).astype(F32),
                )
                spread = jnp.zeros((K_LOC, LANES), F32)
                for q, part in enumerate(parts):
                    spread = jnp.where(lane == K_LOC * q + entry, part, spread)
                at = STEPS * chunks + t
                rows[at : at + 1, :] = jnp.sum(spread, axis=0, keepdims=True)

        tile = rows[...].astype(BF16)
        for d in range(out.shape[0]):
            out[d] = tile


def inner_kernel(order, got, hid, val, ids, out, cvec, idb, vb):
    n = out.shape[0]
    step = hid.shape[0] // n
    chunks = hid.shape[1] // LANES
    lane = lax.broadcasted_iota(jnp.int32, (K_LOC, LANES), 1)
    tile = got[0].astype(F32)
    for d in range(1, got.shape[0]):
        tile = tile + got[d].astype(F32)
    entry = lax.broadcasted_iota(jnp.int32, (K_LOC, LANES), 0)
    cvec[...] = jnp.zeros_like(cvec)
    norms = []
    for t in range(STEPS):
        for j in range(chunks):
            r = t * chunks + j
            cvec[2 + t : 3 + t, j * LANES : (j + 1) * LANES] = tile[r : r + 1, :]
        at = STEPS * chunks + t
        low = jnp.broadcast_to(tile[at : at + 1, :], (K_LOC, LANES))
        cs = [jnp.sum(jnp.where(lane == K_LOC * q + entry, low, 0.0), axis=1, keepdims=True) for q in range(4)]
        idc = (cs[1] * 65536.0 + cs[2] * 256.0 + cs[3]).astype(jnp.int32)
        for l in range(K_LOC):
            idb[t * K_LOC + l] = jnp.broadcast_to(idc[l : l + 1, :], (K_LOC, LANES)).astype(jnp.int16)
            vb[t * K_LOC + l] = jnp.broadcast_to(cs[0][l : l + 1, :], (K_LOC, LANES)).astype(BF16)
        norms.append(jnp.sum(cs[0] * cs[0], axis=0, keepdims=True))
    cmat = cvec[...]
    crow = lax.broadcasted_iota(jnp.int32, (8, LANES), 0)
    tail = jnp.broadcast_to(jnp.sum(cmat * cmat, axis=1, keepdims=True), (8, LANES))
    for t in range(STEPS):
        tail = jnp.where(crow == 2 + STEPS + t, norms[t], tail)
    cb = cmat.astype(BF16)
    srow = lax.broadcasted_iota(jnp.int32, (8, step), 0)
    dims = (((1,), (1,)), ((), ()))
    tiles = step // LANES
    for d in range(n):
        part = slice(d * step, (d + 1) * step)
        acc = lax.dot_general(cb, hid[part, :], dims, preferred_element_type=F32)
        total = None
        for j in range(chunks):
            h = hid[part, j * LANES : (j + 1) * LANES].astype(F32)
            total = h * h if total is None else total + h * h
        squares = [jnp.sum(total[k * LANES : (k + 1) * LANES, :].T, axis=0, keepdims=True) for k in range(tiles)]
        acc = jnp.where(srow == 0, jnp.concatenate(squares, axis=1), acc)
        ident = ids[:, part].astype(jnp.int16)
        vals = val[:, part].astype(F32)
        acc = jnp.where(srow == 1, jnp.sum(vals * vals, axis=0, keepdims=True), acc)
        for t in range(STEPS):
            w = [jnp.zeros((K_LOC, LANES), BF16)] * tiles
            for l in range(K_LOC):
                idl = idb[t * K_LOC + l]
                vl = vb[t * K_LOC + l]
                w = [jnp.where(ident[:, k * LANES : (k + 1) * LANES] == idl, vl, w[k]) for k in range(tiles)]
            w = jnp.concatenate(w, axis=1)
            aa = jnp.sum(w.astype(F32) * vals, axis=0, keepdims=True)
            acc = jnp.where(srow == 2 + STEPS + t, aa, acc)
        slot = order.index(d)
        out[slot, :, 0:step] = acc
        out[slot, :, step:] = tail


def dist_kernel(parts, mind, sums):
    step = mind.shape[1]
    s = parts[0]
    for d in range(1, parts.shape[0]):
        s = s + parts[d]
    sq = s[0:1, 0:step] * s[1:2, 0:step]
    lane = lax.broadcasted_iota(jnp.int32, (1, LANES), 1)
    row = jnp.zeros((1, LANES), F32)
    low = None
    for t in range(STEPS):
        a, b = 2 + t, 2 + STEPS + t
        norm = s[a : a + 1, step : step + 1] * s[b : b + 1, step : step + 1]
        dist = sq + norm - 2.0 * s[a : a + 1, 0:step] * s[b : b + 1, 0:step]
        dist = jnp.maximum(dist, 0.0)
        low = dist if t == 0 else jnp.minimum(low, dist)
        row = jnp.where(lane == t, jnp.sum(low, axis=1, keepdims=True), row)
    mind[...] = low
    sums[...] = jnp.broadcast_to(row, sums.shape)


def pair_kernel(own, other, sums):
    sums[...] = jnp.broadcast_to(own[0:1, :] + other[0:1, :], sums.shape)


def mean_kernel(pool, sums, mind, out, low):
    low[...] = mind[...]
    total = jnp.sum(sums[...], axis=0) / pool
    out[...] = total[0 : out.shape[0]]


def body(hidden_states, factor_values, class_ids, centers):
    rows_all, width = hidden_states.shape
    n_dp, n_mp = lax.axis_size(DP), lax.axis_size(MP)
    n_all = n_dp * n_mp
    rows = rows_all // n_mp
    val = factor_values.T
    ids = class_ids.T
    order = [6, 4, 0, 2, 7, 5, 1, 3]
    hbm = pl.BlockSpec(memory_space=pltpu.HBM)

    picked = pl.pallas_call(
        pick_kernel,
        out_shape=jax.ShapeDtypeStruct((n_dp, 16, LANES), BF16),
        in_specs=[hbm] * 4,
        out_specs=vspec(),
        scratch_shapes=[
            pltpu.SMEM((STEPS,), jnp.int32),
            VMEM((STEPS, 8, width), BF16),
            VMEM((STEPS, K_LOC, LANES), BF16),
            VMEM((STEPS, K_LOC, LANES), jnp.int32),
            VMEM((16, LANES), F32),
            pltpu.SemaphoreType.DMA,
            pltpu.SemaphoreType.DMA((STEPS, 3)),
        ],
        compiler_params=params(4),
    )(*(pltpu.with_memory_space_constraint(x, pltpu.HBM) for x in (centers, hidden_states, val, ids)))
    got = lax.all_to_all(picked, DP, 0, 0, tiled=True, axis_index_groups=[[13, 1, 0, 3, 2, 7, 6, 5, 4, 9, 8, 11, 10, 15, 14, 12]])

    parts = pl.pallas_call(
        functools.partial(inner_kernel, order),
        out_shape=jax.ShapeDtypeStruct((n_mp, 8, rows + LANES), F32),
        in_specs=[vspec()] * 4,
        out_specs=vspec(),
        scratch_shapes=[
            VMEM((8, width), F32),
            VMEM((STEPS * K_LOC, K_LOC, LANES), jnp.int16),
            VMEM((STEPS * K_LOC, K_LOC, LANES), BF16),
        ],
        compiler_params=params(24),
    )(got, hidden_states, val, ids)
    parts = lax.all_to_all(parts, MP, 0, 0, tiled=True, axis_index_groups=[order])

    mind, sums = pl.pallas_call(
        dist_kernel,
        out_shape=[
            VMEM((1, rows), F32),
            jax.ShapeDtypeStruct((1, LANES), F32),
        ],
        in_specs=[vspec()],
        out_specs=[vspec(), vspec()],
        compiler_params=params(4),
    )(parts)
    other = lax.ppermute(sums, "dp_2", [(0, 1), (1, 0)])
    sums = pl.pallas_call(
        pair_kernel,
        out_shape=jax.ShapeDtypeStruct((n_all // 2, LANES), F32),
        in_specs=[vspec(), vspec()],
        out_specs=vspec(),
        compiler_params=params(4),
    )(sums, other)
    sums = lax.all_to_all(sums, ("dp_0", "dp_1", "mp_0", "mp_1"), 0, 0, tiled=True, axis_index_groups=[led_by(n_all // 2, 52)])
    means, mind = pl.pallas_call(
        functools.partial(mean_kernel, rows_all * n_dp),
        out_shape=[jax.ShapeDtypeStruct((STEPS,), F32), jax.ShapeDtypeStruct((1, rows), F32)],
        in_specs=[vspec(), vspec()],
        out_specs=[vspec(), vspec()],
        compiler_params=params(4),
    )(sums, mind)
    return mind.reshape(rows), means


def solution(mesh):
    finer = Mesh(mesh.devices.reshape(2, 4, 2, 4, 2), DP_MP)
    return jax.shard_map(
        body,
        mesh=finer,
        in_specs=(P(DP, MP), P(DP, MP), P(DP, MP), P()),
        out_specs=(P(DP_MP), P()),
        check_vma=False,
    )
```
